32 devices in a mesh: blk: 8 (over z, x), bfly: 4 (over y, core).
Axes of the slice: x: 2, y: 2, z: 4, core: 2. Of those that a mesh axis runs over, the one named last changes fastest.
Arguments:
- port_vectors: bfloat16 [8, 4, 768, 128], P('blk', 'bfly'), may hold values from -6 to 6
- column_leaf: bfloat16 [8, 4, 384, 768], P('blk', 'bfly'), may hold values from -0.21875 to 0.21875
- transfer: bfloat16 [8, 4, 4, 384, 768], P('blk', None, 'bfly'), may hold values from -0.21875 to 0.21875
- row_leaf: bfloat16 [8, 4, 768, 384], P('blk', 'bfly'), may hold values from -0.3125 to 0.3125
Outputs:
- field: bfloat16 [4, 768, 128], P('bfly', 'blk')
The draws below stay inside these ranges and needn't reach their ends.
All inputs are finite; a program needn't handle non-finite values.
Results may differ from the reference program's by a relative error of at most 0.0095.
Values may be sent and summed in bfloat16 or wider, within the bound.
A program may use at most 64 MiB of HBM per device.

```python
import math
import jax
import jax.numpy as jnp
import numpy as np
from jax import lax

RANK = 384
LEAF = 768
PORTS = 128
LEVELS = 4
BLOCKS = 8
N_BLK = 8
N_BFLY = 4


def steps_of(stream_key, dims, pieces, smallest, high):
    gain = 1.0
    for axis_at, parts in pieces:
        steps = jax.random.uniform(jax.random.fold_in(jax.random.fold_in(stream_key, 6), axis_at), (parts,), jnp.float32, smallest / len(pieces), high / len(pieces))
        gain = gain * jnp.repeat(jnp.exp(steps), dims[axis_at] // parts).reshape((-1,) + (1,) * (len(dims) - 1 - axis_at))
    return gain


def bell_draw(rng, shape, scale, reach, split=(), kind=jnp.bfloat16):
    array = scale * jax.random.normal(rng, shape, jnp.float32)
    if split:
        array = array * steps_of(rng, shape, split, -0.22, 0.18)
    return jnp.clip(array, -reach, reach).astype(kind)


def setup_inputs(seed: int = 0) -> dict:
    seeds = jax.random.split(jax.random.key(seed), 5)
    return {
        "port_vectors": bell_draw(seeds[0], (BLOCKS, N_BFLY, LEAF, PORTS), 1.0, 6.0, ((0, 8), (1, 4))),
        "column_leaf": bell_draw(seeds[1], (BLOCKS, N_BFLY, RANK, LEAF), LEAF ** -0.5, 0.21875, ((0, 8), (1, 4))),
        "transfer": bell_draw(seeds[2], (BLOCKS, LEVELS, N_BFLY, RANK, 2 * RANK), (2 * RANK) ** -0.5, 0.21875, ((0, 8), (2, 4))),
        "row_leaf": bell_draw(seeds[3], (BLOCKS, N_BFLY, LEAF, RANK), RANK ** -0.5, 0.3125, ((0, 8), (1, 4))),
    }


def reference(port_vectors, column_leaf, transfer, row_leaf):
    bit_count = N_BFLY.bit_length() - 1
    positions = np.arange(N_BFLY)

    def one_block(total, items):
        ports, cleaf, trans, rleaf = items
        state = jnp.einsum('pkl,plr->pkr', cleaf.astype(jnp.float32), ports.astype(jnp.float32)).astype(jnp.bfloat16)
        for level in range(LEVELS):
            stride = 1 << level % bit_count
            lower = jnp.asarray(positions & ~stride, dtype=jnp.int32)
            upper = jnp.asarray(positions | stride, dtype=jnp.int32)
            stacked = jnp.concatenate([state[lower], state[upper]], axis=1)
            state = jnp.einsum('pkj,pjr->pkr', trans[level].astype(jnp.float32), stacked.astype(jnp.float32)).astype(jnp.bfloat16)
        partial_rows = jnp.einsum('plk,pkr->plr', rleaf.astype(jnp.float32), state.astype(jnp.float32))
        return (total + partial_rows, None)
    start = jnp.zeros((N_BFLY, LEAF, PORTS), jnp.float32)
    total, _ = lax.scan(one_block, start, (port_vectors, column_leaf, transfer, row_leaf))
    return (total * (1.0 / math.sqrt(N_BLK))).astype(jnp.bfloat16)
```

```python
import functools
import math

import jax
import jax.numpy as jnp
from jax import lax
from jax.experimental import pallas as pl
from jax.experimental.pallas import tpu as pltpu
from jax.sharding import PartitionSpec as P

PIECES = 2
MESH = pl.DeviceIdType.MESH
F32 = jnp.float32
BF16 = jnp.bfloat16


def plan(levels, bit_count):
    bits = [level % bit_count for level in range(levels)]
    stages, level = [], 1
    while level < levels - 1:
        assert bits[level] > 0
        pair = level + 1 < levels - 1 and bits[level + 1] == 0
        stages.append((level, level + 1) if pair else (level,))
        level += len(stages[-1])
    assert stages and bits[levels - 1] > 0
    return bits, stages


def contract(left, right):
    return lax.dot_general(left, right, (((1,), (1,)), ((), ())), preferred_element_type=F32)


def kernel(
    n_blk, n_bfly, pieces,
    ports_hbm, column_hbm, transfer_hbm, row_hbm, out_ref,
    ports, column, transfer, foreign, row, first, held, arrived, begun, turned, mixing, lent,
    last, outgoing, incoming, merged, partial,
    load_sem, row_sem, first_sem, weight_send, weight_recv, held_sem,
    stage_send, stage_recv, last_send, last_recv, down_send, down_recv, scatter_send, scatter_recv,
):
    levels, rank, _ = transfer.shape
    count = ports.shape[1]
    leaf = row.shape[0]
    owned = leaf // n_blk
    bits, stages = plan(levels, n_bfly.bit_length() - 1)
    entry, final = stages[0][0], levels - 1
    block = lax.axis_index("blk")
    position = lax.axis_index("bfly")
    core = lax.rem(position, 2)
    host, helper = core == 1, core == 0
    width = count // pieces
    spans = [pl.ds(piece * width, width) for piece in range(pieces)]
    group = owned // pieces

    def load(source, target, sem):
        copy = pltpu.make_async_copy(source, target, sem)
        copy.start()
        return copy

    loads = [
        load(ports_hbm.at[0, 0], ports, load_sem.at[levels]),
        load(column_hbm.at[0, 0], column, load_sem.at[levels + 1]),
    ]
    transfer_loads = [
        load(transfer_hbm.at[0, level, 0], transfer.at[level], load_sem.at[level])
        for level in [0, 1, levels - 1] + list(range(2, levels - 1))
    ]
    transfer_loads = {
        level: copy
        for level, copy in zip([0, 1, levels - 1] + list(range(2, levels - 1)), transfer_loads)
    }
    row_loads = []
    for slot in range(n_blk):
        owner = block ^ (n_blk - 1 - slot)
        row_loads.append(
            load(
                row_hbm.at[0, 0, pl.ds(pl.multiple_of(owner * owned, owned), owned)],
                row.at[pl.ds(slot * owned, owned)],
                row_sem.at[slot],
            )
        )

    def side(which):
        return pl.ds(pl.multiple_of(which * rank, rank), rank)

    def bit_of(level):
        return lax.rem(position // 2 ** bits[level], 2)

    def across(level, to_core):
        place = position + (1 - 2 * bit_of(level)) * 2 ** bits[level]
        return {"bfly": place - core + to_core}

    mate = {"bfly": position + 1 - 2 * core}
    barrier = pltpu.get_barrier_semaphore()

    def greet(target):
        pl.semaphore_signal(barrier, inc=1, device_id=target, device_id_type=MESH)

    host_bits = {}
    for level in [stage[0] for stage in stages] + [final]:
        host_bits.setdefault(bits[level], level)
    mixed_bits = {bits[final]: final, bits[entry]: entry}
    greet(mate)
    for level in mixed_bits.values():
        greet(across(level, 1 - core))

    @pl.when(host)
    def _():
        for level in host_bits.values():
            greet(across(level, 1))

    for step in range(1, n_blk):
        greet({"blk": block ^ step})

    def remote(source, target, send_sem, recv_sem, device):
        return pltpu.make_async_remote_copy(
            src_ref=source, dst_ref=target, send_sem=send_sem, recv_sem=recv_sem,
            device_id=device, device_id_type=MESH,
        )

    first_copy = remote(first.at[core], first.at[core], first_sem.at[0], first_sem.at[1], mate)
    weight_copies = [
        remote(
            transfer.at[1 + index], foreign.at[index], weight_send.at[index], weight_recv.at[index], mate
        )
        for index in range(levels - 2)
    ]
    held_copy = remote(held.at[0, 0], held.at[0, 0], held_sem.at[0], held_sem.at[1], mate)

    def stage_copy(index, which, piece):
        return remote(
            held.at[index, which, spans[piece]], arrived.at[index, which, spans[piece]],
            stage_send.at[index, which, piece], stage_recv.at[index, which, piece],
            across(stages[index][0], 1),
        )

    mine = bit_of(final)

    def last_copy(which, piece):
        source = lent.at[spans[piece]] if which == 0 else last.at[mine, spans[piece]]
        return remote(
            source, last.at[mine, spans[piece]], last_send.at[which, piece], last_recv.at[piece],
            across(final, which),
        )

    def down_copy(piece):
        return remote(
            lent.at[spans[piece]], last.at[mine, spans[piece]], down_send.at[piece],
            down_recv.at[piece], mate,
        )

    def scatter_copy(piece, slot):
        return remote(
            outgoing.at[piece, slot], incoming.at[piece, slot],
            scatter_send.at[piece, slot], scatter_recv.at[piece, slot],
            {"blk": block ^ (n_blk - 1 - slot)},
        )

    def rows(which, piece):
        value = last[which, spans[piece], :]
        return contract(merged[:, side(which)], jnp.concatenate([value] * pieces, axis=0))

    loads[0].wait()
    loads[1].wait()
    state = jnp.dot(column[...], ports[...], preferred_element_type=F32)
    first[core] = state.T.astype(BF16)
    pl.semaphore_wait(barrier, len(mixed_bits) + n_blk + core * len(host_bits))
    first_copy.start()
    transfer_loads[1].wait()

    @pl.when(helper)
    def _():
        weight_copies[0].start()

    transfer_loads[0].wait()
    own = contract(first[core], transfer[0, :, side(core)])
    transfer_loads[final].wait()
    for copy in row_loads:
        copy.wait()
    merged[...] = jnp.dot(row[...], transfer[final], preferred_element_type=F32).astype(BF16)
    first_copy.wait_recv()
    state = own + contract(first[1 - core], transfer[0, :, side(1 - core)])
    held[0, core] = state.astype(BF16)
    for piece in range(pieces):
        stage_copy(0, core, piece).start()
    for level in range(2, final):
        transfer_loads[level].wait()

    @pl.when(helper)
    def _():
        held_copy.start()
        for copy in weight_copies[1:]:
            copy.start()
        for piece in range(pieces):
            down_copy(piece).wait_recv()
            partial[piece] = rows(mine, piece)

    def weights(level, which):
        return transfer.at[level] if which else foreign.at[level - 1]

    def mix(index, states, incoming_side):
        stage = stages[index]
        if len(stage) == 2:
            joined = jnp.concatenate(states, axis=1)
            return jnp.dot(joined, mixing[incoming_side], preferred_element_type=F32)
        which = bit_of(stage[0]) if incoming_side == 0 else 1 - bit_of(stage[0])
        return jnp.concatenate(
            [contract(states[c], weights(stage[0], c)[:, side(which)]) for c in range(2)], axis=1
        )

    def prepare(stage):
        low, high = stage
        bit = bit_of(low)
        for inner in (1, 0):
            if inner == 0:
                weight_copies[low - 1].wait_recv()
            for half, which in ((0, bit), (1, 1 - bit)):
                turned[inner, half] = weights(low, inner)[:, side(which)].T
                mixing[half, inner * rank : (inner + 1) * rank, rank:] = contract(
                    turned[inner, half], weights(high, 1)[:, inner * rank : (inner + 1) * rank]
                ).astype(BF16)
        weight_copies[high - 1].wait_recv()
        for inner in (0, 1):
            for half in range(2):
                mixing[half, inner * rank : (inner + 1) * rank, :rank] = contract(
                    turned[inner, half], weights(high, 0)[:, inner * rank : (inner + 1) * rank]
                ).astype(BF16)

    @pl.when(host)
    def _():
        for index, stage in enumerate(stages):
            if len(stage) == 2:
                prepare(stage)
            else:
                weight_copies[stage[0] - 1].wait_recv()
            if index == 0:
                held_copy.wait_recv()
            begun[...] = mix(index, [held[index, 0], held[index, 1]], 0)
            for piece in range(pieces):
                for which in range(2):
                    stage_copy(index, which, piece).wait_recv()
                total = begun[spans[piece], :] + mix(
                    index, [arrived[index, 0, spans[piece], :], arrived[index, 1, spans[piece], :]], 1
                )
                total = total.astype(BF16)
                if index + 1 < len(stages):
                    for which in range(2):
                        held[index + 1, which, spans[piece], :] = total[:, which * rank : (which + 1) * rank]
                        stage_copy(index + 1, which, piece).start()
                else:
                    lent[spans[piece], :] = total[:, :rank]
                    last_copy(0, piece).start()
                    last[mine, spans[piece], :] = total[:, rank:]
                    last_copy(1, piece).start()
                    down_copy(piece).start()
                    partial[piece] = rows(mine, piece)

    lane = lax.broadcasted_iota(jnp.int32, (group, count), 1)

    def choose(values):
        result = values[0]
        for k in range(1, pieces):
            result = jnp.where(lane < k * width, result, values[k])
        return result

    for piece in range(pieces):
        last_copy(1, piece).wait_recv()
        total = partial[piece] + rows(1 - mine, piece)
        for slot in range(n_blk):
            packed = choose(
                [
                    total[slot * owned + g * group : slot * owned + (g + 1) * group]
                    for g in ((k - piece) % pieces for k in range(pieces))
                ]
            )
            outgoing[piece, slot] = packed.astype(BF16)
            if slot < n_blk - 1:
                scatter_copy(piece, slot).start()

    sums = []
    for piece in range(pieces):
        total = outgoing[piece, n_blk - 1].astype(F32)
        for slot in range(n_blk - 2, -1, -1):
            scatter_copy(piece, slot).wait_recv()
            total = total + incoming[piece, slot].astype(F32)
        sums.append(total * (1.0 / math.sqrt(n_blk)))
    for g in range(pieces):
        value = choose([sums[(k - g) % pieces] for k in range(pieces)])
        if g:
            value = pltpu.roll(value, (count - g * width) % count, 1)
        out_ref[0, g * group : (g + 1) * group, :] = value.astype(BF16)

    first_copy.wait_send()
    for piece in range(pieces):
        stage_copy(0, core, piece).wait_send()
        for slot in range(n_blk - 1):
            scatter_copy(piece, slot).wait_send()

    @pl.when(helper)
    def _():
        held_copy.wait_send()
        for copy in weight_copies:
            copy.wait_send()

    @pl.when(host)
    def _():
        for piece in range(pieces):
            for index in range(1, len(stages)):
                for which in range(2):
                    stage_copy(index, which, piece).wait_send()
            last_copy(0, piece).wait_send()
            last_copy(1, piece).wait_send()
            down_copy(piece).wait_send()


def solution(mesh):
    n_blk, n_bfly = mesh.shape["blk"], mesh.shape["bfly"]

    def local(port_vectors, column_leaf, transfer, row_leaf):
        _, _, leaf, ports = port_vectors.shape
        rank = column_leaf.shape[2]
        levels = transfer.shape[1]
        rows = row_leaf.shape[2]
        owned = rows // n_blk
        _, stages = plan(levels, n_bfly.bit_length() - 1)
        assert n_blk & (n_blk - 1) == 0
        dma = pltpu.SemaphoreType.DMA
        return pl.pallas_call(
            functools.partial(kernel, n_blk, n_bfly, PIECES),
            out_shape=pltpu.VMEM((1, owned, ports), BF16),
            in_specs=[pl.BlockSpec(memory_space=pl.ANY)] * 4,
            out_specs=pl.BlockSpec(memory_space=pltpu.VMEM),
            scratch_shapes=[
                pltpu.VMEM((leaf, ports), BF16),
                pltpu.VMEM((rank, leaf), BF16),
                pltpu.VMEM((levels, rank, 2 * rank), BF16),
                pltpu.VMEM((levels - 2, rank, 2 * rank), BF16),
                pltpu.VMEM((rows, rank), BF16),
                pltpu.VMEM((2, ports, rank), BF16),
                pltpu.VMEM((len(stages), 2, ports, rank), BF16),
                pltpu.VMEM((len(stages), 2, ports, rank), BF16),
                pltpu.VMEM((ports, 2 * rank), F32),
                pltpu.VMEM((2, 2, rank, rank), BF16),
                pltpu.VMEM((2, 2 * rank, 2 * rank), BF16),
                pltpu.VMEM((ports, rank), BF16),
                pltpu.VMEM((2, ports, rank), BF16),
                pltpu.VMEM((PIECES, n_blk, owned // PIECES, ports), BF16),
                pltpu.VMEM((PIECES, n_blk, owned // PIECES, ports), BF16),
                pltpu.VMEM((rows, 2 * rank), BF16),
                pltpu.VMEM((PIECES, rows, ports), F32),
                dma((levels + 2,)),
                dma((n_blk,)),
                dma((2,)),
                dma((levels - 2,)),
                dma((levels - 2,)),
                dma((2,)),
                dma((len(stages), 2, PIECES)),
                dma((len(stages), 2, PIECES)),
                dma((2, PIECES)),
                dma((PIECES,)),
                dma((PIECES,)),
                dma((PIECES,)),
                dma((PIECES, n_blk)),
                dma((PIECES, n_blk)),
            ],
            compiler_params=pltpu.CompilerParams(collective_id=0, has_side_effects=True),
        )(port_vectors, column_leaf, transfer, row_leaf)

    placed = (
        P("blk", "bfly", None, None),
        P("blk", "bfly", None, None),
        P("blk", None, "bfly", None, None),
        P("blk", "bfly", None, None),
    )
    return jax.shard_map(
        local, mesh=mesh, in_specs=placed, out_specs=P("bfly", "blk", None), check_vma=False
    )
```

```python
import functools
import math

import jax
import jax.numpy as jnp
from jax import lax
from jax.experimental import pallas as pl
from jax.experimental.pallas import tpu as pltpu
from jax.sharding import PartitionSpec as P

PIECES = 2
MESH = pl.DeviceIdType.MESH
F32 = jnp.float32
BF16 = jnp.bfloat16


def plan(levels, bit_count):
    bits = [level % bit_count for level in range(levels)]
    stages, level = [], 1
    while level < levels - 1:
        assert bits[level] > 0
        pair = level + 1 < levels - 1 and bits[level + 1] == 0
        stages.append((level, level + 1) if pair else (level,))
        level += len(stages[-1])
    assert stages and bits[levels - 1] > 0
    return bits, stages


def contract(left, right):
    return lax.dot_general(left, right, (((1,), (1,)), ((), ())), preferred_element_type=F32)


def kernel(
    n_blk, n_bfly, pieces,
    ports_hbm, column_hbm, transfer_hbm, row_hbm, out_ref,
    ports, column, transfer, foreign, row, first, held, arrived, begun, turned, mixing, lent,
    last, outgoing, incoming, merged, partial,
    load_sem, row_sem, first_sem, weight_send, weight_recv, held_sem,
    stage_send, stage_recv, last_send, last_recv, down_send, down_recv, scatter_send, scatter_recv,
    meet_sem,
):
    levels, rank, _ = transfer.shape
    count = ports.shape[1]
    leaf = row.shape[0]
    owned = leaf // n_blk
    bits, stages = plan(levels, n_bfly.bit_length() - 1)
    entry, final = stages[0][0], levels - 1
    block = lax.axis_index("blk")
    position = lax.axis_index("bfly")
    core = lax.rem(position, 2)
    host, helper = core == 1, core == 0
    width = count // pieces
    spans = [pl.ds(piece * width, width) for piece in range(pieces)]
    group = owned // pieces

    def load(source, target, sem):
        copy = pltpu.make_async_copy(source, target, sem)
        copy.start()
        return copy

    loads = [
        load(ports_hbm.at[0, 0], ports, load_sem.at[levels]),
        load(column_hbm.at[0, 0], column, load_sem.at[levels + 1]),
    ]
    transfer_loads = [
        load(transfer_hbm.at[0, level, 0], transfer.at[level], load_sem.at[level])
        for level in [0, 1, levels - 1] + list(range(2, levels - 1))
    ]
    transfer_loads = {
        level: copy
        for level, copy in zip([0, 1, levels - 1] + list(range(2, levels - 1)), transfer_loads)
    }
    row_loads = []
    for slot in range(n_blk):
        owner = block ^ (n_blk - 1 - slot)
        row_loads.append(
            load(
                row_hbm.at[0, 0, pl.ds(pl.multiple_of(owner * owned, owned), owned)],
                row.at[pl.ds(slot * owned, owned)],
                row_sem.at[slot],
            )
        )

    def side(which):
        return pl.ds(pl.multiple_of(which * rank, rank), rank)

    def bit_of(level):
        return lax.rem(position // 2 ** bits[level], 2)

    def across(level, to_core):
        place = position + (1 - 2 * bit_of(level)) * 2 ** bits[level]
        return {"bfly": place - core + to_core}

    mate = {"bfly": position + 1 - 2 * core}
    barrier = pltpu.get_barrier_semaphore()

    def greet(target):
        pl.semaphore_signal(barrier, inc=1, device_id=target, device_id_type=MESH)

    host_bits = {}
    for level in [stage[0] for stage in stages] + [final]:
        host_bits.setdefault(bits[level], level)
    mixed_bits = {bits[final]: final, bits[entry]: entry}
    greet(mate)
    for level in mixed_bits.values():
        greet(across(level, 1 - core))

    @pl.when(host)
    def _():
        for level in host_bits.values():
            greet(across(level, 1))

    blk_bits = n_blk.bit_length() - 1
    for bit in range(blk_bits):
        greet({"blk": block ^ (1 << bit)})

    def tell(turn):
        if turn < blk_bits - 1:
            for bit in range(blk_bits):
                pl.semaphore_signal(
                    meet_sem.at[turn, bit], inc=1, device_id={"blk": block ^ (1 << bit)},
                    device_id_type=MESH,
                )

    def hear(turn):
        if turn < blk_bits - 1:
            for bit in range(blk_bits):
                pl.semaphore_wait(meet_sem.at[turn, bit], 1)

    def remote(source, target, send_sem, recv_sem, device):
        return pltpu.make_async_remote_copy(
            src_ref=source, dst_ref=target, send_sem=send_sem, recv_sem=recv_sem,
            device_id=device, device_id_type=MESH,
        )

    first_copy = remote(first.at[core], first.at[core], first_sem.at[0], first_sem.at[1], mate)
    weight_copies = [
        remote(
            transfer.at[1 + index], foreign.at[index], weight_send.at[index], weight_recv.at[index], mate
        )
        for index in range(levels - 2)
    ]
    held_copy = remote(held.at[0, 0], held.at[0, 0], held_sem.at[0], held_sem.at[1], mate)

    def stage_copy(index, which, piece):
        return remote(
            held.at[index, which, spans[piece]], arrived.at[index, which, spans[piece]],
            stage_send.at[index, which, piece], stage_recv.at[index, which, piece],
            across(stages[index][0], 1),
        )

    mine = bit_of(final)

    def last_copy(which, piece):
        source = lent.at[spans[piece]] if which == 0 else last.at[mine, spans[piece]]
        return remote(
            source, last.at[mine, spans[piece]], last_send.at[which, piece], last_recv.at[piece],
            across(final, which),
        )

    def down_copy(piece):
        return remote(
            lent.at[spans[piece]], last.at[mine, spans[piece]], down_send.at[piece],
            down_recv.at[piece], mate,
        )

    def scatter_copy(piece, slot):
        return remote(
            outgoing.at[piece, slot], incoming.at[piece, slot],
            scatter_send.at[piece, slot], scatter_recv.at[piece, slot],
            {"blk": block ^ (n_blk - 1 - slot)},
        )

    def rows(which, piece):
        value = last[which, spans[piece], :]
        return contract(merged[:, side(which)], jnp.concatenate([value] * pieces, axis=0))

    loads[0].wait()
    loads[1].wait()
    state = jnp.dot(column[...], ports[...], preferred_element_type=F32)
    first[core] = state.T.astype(BF16)
    pl.semaphore_wait(barrier, 1 + len(mixed_bits) + blk_bits + core * len(host_bits))
    tell(0)
    first_copy.start()
    transfer_loads[1].wait()

    @pl.when(helper)
    def _():
        weight_copies[0].start()

    transfer_loads[0].wait()
    own = contract(first[core], transfer[0, :, side(core)])
    transfer_loads[final].wait()
    for copy in row_loads:
        copy.wait()
    merged[...] = jnp.dot(row[...], transfer[final], preferred_element_type=F32).astype(BF16)
    first_copy.wait_recv()
    state = own + contract(first[1 - core], transfer[0, :, side(1 - core)])
    held[0, core] = state.astype(BF16)
    for piece in range(pieces):
        stage_copy(0, core, piece).start()
    hear(0)
    tell(1)
    for level in range(2, final):
        transfer_loads[level].wait()

    @pl.when(helper)
    def _():
        held_copy.start()
        for copy in weight_copies[1:]:
            copy.start()
        for piece in range(pieces):
            down_copy(piece).wait_recv()
            partial[piece] = rows(mine, piece)

    def weights(level, which):
        return transfer.at[level] if which else foreign.at[level - 1]

    def mix(index, states, incoming_side):
        stage = stages[index]
        if len(stage) == 2:
            joined = jnp.concatenate(states, axis=1)
            return jnp.dot(joined, mixing[incoming_side], preferred_element_type=F32)
        which = bit_of(stage[0]) if incoming_side == 0 else 1 - bit_of(stage[0])
        return jnp.concatenate(
            [contract(states[c], weights(stage[0], c)[:, side(which)]) for c in range(2)], axis=1
        )

    def prepare(stage):
        low, high = stage
        bit = bit_of(low)
        for inner in (1, 0):
            if inner == 0:
                weight_copies[low - 1].wait_recv()
            for half, which in ((0, bit), (1, 1 - bit)):
                turned[inner, half] = weights(low, inner)[:, side(which)].T
                mixing[half, inner * rank : (inner + 1) * rank, rank:] = contract(
                    turned[inner, half], weights(high, 1)[:, inner * rank : (inner + 1) * rank]
                ).astype(BF16)
        weight_copies[high - 1].wait_recv()
        for inner in (0, 1):
            for half in range(2):
                mixing[half, inner * rank : (inner + 1) * rank, :rank] = contract(
                    turned[inner, half], weights(high, 0)[:, inner * rank : (inner + 1) * rank]
                ).astype(BF16)

    @pl.when(host)
    def _():
        for index, stage in enumerate(stages):
            if len(stage) == 2:
                prepare(stage)
            else:
                weight_copies[stage[0] - 1].wait_recv()
            if index == 0:
                held_copy.wait_recv()
            begun[...] = mix(index, [held[index, 0], held[index, 1]], 0)
            for piece in range(pieces):
                for which in range(2):
                    stage_copy(index, which, piece).wait_recv()
                total = begun[spans[piece], :] + mix(
                    index, [arrived[index, 0, spans[piece], :], arrived[index, 1, spans[piece], :]], 1
                )
                total = total.astype(BF16)
                if index + 1 < len(stages):
                    for which in range(2):
                        held[index + 1, which, spans[piece], :] = total[:, which * rank : (which + 1) * rank]
                        stage_copy(index + 1, which, piece).start()
                else:
                    lent[spans[piece], :] = total[:, :rank]
                    last_copy(0, piece).start()
                    last[mine, spans[piece], :] = total[:, rank:]
                    last_copy(1, piece).start()
                    down_copy(piece).start()
                    partial[piece] = rows(mine, piece)

    for turn in range(1, blk_bits - 1):
        hear(turn)
        tell(turn + 1)
    lane = lax.broadcasted_iota(jnp.int32, (group, count), 1)

    def choose(values):
        result = values[0]
        for k in range(1, pieces):
            result = jnp.where(lane < k * width, result, values[k])
        return result

    for piece in range(pieces):
        last_copy(1, piece).wait_recv()
        total = partial[piece] + rows(1 - mine, piece)
        for slot in range(n_blk):
            packed = choose(
                [
                    total[slot * owned + g * group : slot * owned + (g + 1) * group]
                    for g in ((k - piece) % pieces for k in range(pieces))
                ]
            )
            outgoing[piece, slot] = packed.astype(BF16)
            if slot < n_blk - 1:
                scatter_copy(piece, slot).start()

    sums = []
    for piece in range(pieces):
        total = outgoing[piece, n_blk - 1].astype(F32)
        for slot in range(n_blk - 2, -1, -1):
            scatter_copy(piece, slot).wait_recv()
            total = total + incoming[piece, slot].astype(F32)
        sums.append(total * (1.0 / math.sqrt(n_blk)))
    for g in range(pieces):
        value = choose([sums[(k - g) % pieces] for k in range(pieces)])
        if g:
            value = pltpu.roll(value, (count - g * width) % count, 1)
        out_ref[0, g * group : (g + 1) * group, :] = value.astype(BF16)

    first_copy.wait_send()
    for piece in range(pieces):
        stage_copy(0, core, piece).wait_send()
        for slot in range(n_blk - 1):
            scatter_copy(piece, slot).wait_send()

    @pl.when(helper)
    def _():
        held_copy.wait_send()
        for copy in weight_copies:
            copy.wait_send()

    @pl.when(host)
    def _():
        for piece in range(pieces):
            for index in range(1, len(stages)):
                for which in range(2):
                    stage_copy(index, which, piece).wait_send()
            last_copy(0, piece).wait_send()
            last_copy(1, piece).wait_send()
            down_copy(piece).wait_send()


def solution(mesh):
    n_blk, n_bfly = mesh.shape["blk"], mesh.shape["bfly"]

    def local(port_vectors, column_leaf, transfer, row_leaf):
        _, _, leaf, ports = port_vectors.shape
        rank = column_leaf.shape[2]
        levels = transfer.shape[1]
        rows = row_leaf.shape[2]
        owned = rows // n_blk
        _, stages = plan(levels, n_bfly.bit_length() - 1)
        assert n_blk & (n_blk - 1) == 0
        dma = pltpu.SemaphoreType.DMA
        return pl.pallas_call(
            functools.partial(kernel, n_blk, n_bfly, PIECES),
            out_shape=pltpu.VMEM((1, owned, ports), BF16),
            in_specs=[pl.BlockSpec(memory_space=pl.ANY)] * 4,
            out_specs=pl.BlockSpec(memory_space=pltpu.VMEM),
            scratch_shapes=[
                pltpu.VMEM((leaf, ports), BF16),
                pltpu.VMEM((rank, leaf), BF16),
                pltpu.VMEM((levels, rank, 2 * rank), BF16),
                pltpu.VMEM((levels - 2, rank, 2 * rank), BF16),
                pltpu.VMEM((rows, rank), BF16),
                pltpu.VMEM((2, ports, rank), BF16),
                pltpu.VMEM((len(stages), 2, ports, rank), BF16),
                pltpu.VMEM((len(stages), 2, ports, rank), BF16),
                pltpu.VMEM((ports, 2 * rank), F32),
                pltpu.VMEM((2, 2, rank, rank), BF16),
                pltpu.VMEM((2, 2 * rank, 2 * rank), BF16),
                pltpu.VMEM((ports, rank), BF16),
                pltpu.VMEM((2, ports, rank), BF16),
                pltpu.VMEM((PIECES, n_blk, owned // PIECES, ports), BF16),
                pltpu.VMEM((PIECES, n_blk, owned // PIECES, ports), BF16),
                pltpu.VMEM((rows, 2 * rank), BF16),
                pltpu.VMEM((PIECES, rows, ports), F32),
                dma((levels + 2,)),
                dma((n_blk,)),
                dma((2,)),
                dma((levels - 2,)),
                dma((levels - 2,)),
                dma((2,)),
                dma((len(stages), 2, PIECES)),
                dma((len(stages), 2, PIECES)),
                dma((2, PIECES)),
                dma((PIECES,)),
                dma((PIECES,)),
                dma((PIECES,)),
                dma((PIECES, n_blk)),
                dma((PIECES, n_blk)),
                pltpu.SemaphoreType.REGULAR((n_blk.bit_length(), n_blk.bit_length())),
            ],
            compiler_params=pltpu.CompilerParams(collective_id=0, has_side_effects=True),
        )(port_vectors, column_leaf, transfer, row_leaf)

    placed = (
        P("blk", "bfly", None, None),
        P("blk", "bfly", None, None),
        P("blk", None, "bfly", None, None),
        P("blk", "bfly", None, None),
    )
    return jax.shard_map(
        local, mesh=mesh, in_specs=placed, out_specs=P("bfly", "blk", None), check_vma=False
    )
```

```python
import functools
import math

import jax
import jax.numpy as jnp
from jax import lax
from jax.experimental import pallas as pl
from jax.experimental.pallas import tpu as pltpu
from jax.sharding import PartitionSpec as P

PIECES = 4
MESH = pl.DeviceIdType.MESH
F32 = jnp.float32
BF16 = jnp.bfloat16


def plan(levels, bit_count):
    bits = [level % bit_count for level in range(levels)]
    stages, level = [], 1
    while level < levels - 1:
        assert bits[level] > 0
        pair = level + 1 < levels - 1 and bits[level + 1] == 0
        stages.append((level, level + 1) if pair else (level,))
        level += len(stages[-1])
    assert stages and bits[levels - 1] > 0
    return bits, stages


def contract(left, right):
    return lax.dot_general(left, right, (((1,), (1,)), ((), ())), preferred_element_type=F32)


def kernel(
    n_blk, n_bfly, pieces,
    ports_hbm, column_hbm, transfer_hbm, row_hbm, out_ref,
    ports, column, transfer, foreign, row, first, held, arrived, begun, turned, mixing, lent,
    last, outgoing, incoming, merged, partial,
    load_sem, row_sem, first_sem, weight_send, weight_recv, held_sem,
    stage_send, stage_recv, last_send, last_recv, down_send, down_recv, scatter_send, scatter_recv,
    meet_sem,
):
    levels, rank, _ = transfer.shape
    count = ports.shape[1]
    leaf = row.shape[0]
    owned = leaf // n_blk
    bits, stages = plan(levels, n_bfly.bit_length() - 1)
    entry, final = stages[0][0], levels - 1
    block = lax.axis_index("blk")
    position = lax.axis_index("bfly")
    core = lax.rem(position, 2)
    host, helper = core == 1, core == 0
    width = count // pieces
    spans = [pl.ds(piece * width, width) for piece in range(pieces)]
    group = owned // pieces

    def load(source, target, sem):
        copy = pltpu.make_async_copy(source, target, sem)
        copy.start()
        return copy

    loads = [
        load(ports_hbm.at[0, 0], ports, load_sem.at[levels]),
        load(column_hbm.at[0, 0], column, load_sem.at[levels + 1]),
    ]
    transfer_loads = {
        level: load(transfer_hbm.at[0, level, 0], transfer.at[level], load_sem.at[level])
        for level in range(levels)
    }
    row_loads = []
    for slot in range(n_blk):
        owner = block ^ (n_blk - 1 - slot)
        row_loads.append(
            load(
                row_hbm.at[0, 0, pl.ds(pl.multiple_of(owner * owned, owned), owned)],
                row.at[pl.ds(slot * owned, owned)],
                row_sem.at[slot],
            )
        )

    def side(which):
        return pl.ds(pl.multiple_of(which * rank, rank), rank)

    def bit_of(level):
        return lax.rem(position // 2 ** bits[level], 2)

    def across(level, to_core):
        place = position + (1 - 2 * bit_of(level)) * 2 ** bits[level]
        return {"bfly": place - core + to_core}

    mate = {"bfly": position + 1 - 2 * core}
    barrier = pltpu.get_barrier_semaphore()

    def greet(target):
        pl.semaphore_signal(barrier, inc=1, device_id=target, device_id_type=MESH)

    host_bits = {}
    for level in [stage[0] for stage in stages] + [final]:
        host_bits.setdefault(bits[level], level)
    mixed_bits = {bits[final]: final, bits[entry]: entry}
    greet(mate)
    for level in mixed_bits.values():
        greet(across(level, 1 - core))

    @pl.when(host)
    def _():
        for level in host_bits.values():
            greet(across(level, 1))

    blk_bits = n_blk.bit_length() - 1
    for bit in range(blk_bits):
        greet({"blk": block ^ (1 << bit)})

    def tell(turn):
        if turn < blk_bits - 1:
            for bit in range(blk_bits):
                pl.semaphore_signal(
                    meet_sem.at[turn, bit], inc=1, device_id={"blk": block ^ (1 << bit)},
                    device_id_type=MESH,
                )

    def hear(turn):
        if turn < blk_bits - 1:
            for bit in range(blk_bits):
                pl.semaphore_wait(meet_sem.at[turn, bit], 1)

    def remote(source, target, send_sem, recv_sem, device):
        return pltpu.make_async_remote_copy(
            src_ref=source, dst_ref=target, send_sem=send_sem, recv_sem=recv_sem,
            device_id=device, device_id_type=MESH,
        )

    first_copy = remote(first.at[core], first.at[core], first_sem.at[0], first_sem.at[1], mate)
    weight_copies = [
        remote(
            transfer.at[1 + index], foreign.at[index], weight_send.at[index], weight_recv.at[index], mate
        )
        for index in range(levels - 2)
    ]
    held_copy = remote(held.at[0, 0], held.at[0, 0], held_sem.at[0], held_sem.at[1], mate)

    def stage_copy(index, which, piece):
        return remote(
            held.at[index, which, spans[piece]], arrived.at[index, which, spans[piece]],
            stage_send.at[index, which, piece], stage_recv.at[index, which, piece],
            across(stages[index][0], 1),
        )

    mine = bit_of(final)

    def last_copy(which, piece):
        source = lent.at[spans[piece]] if which == 0 else last.at[mine, spans[piece]]
        return remote(
            source, last.at[mine, spans[piece]], last_send.at[which, piece], last_recv.at[piece],
            across(final, which),
        )

    def down_copy(piece):
        return remote(
            lent.at[spans[piece]], last.at[mine, spans[piece]], down_send.at[piece],
            down_recv.at[piece], mate,
        )

    def scatter_copy(piece, slot):
        return remote(
            outgoing.at[piece, slot], incoming.at[piece, slot],
            scatter_send.at[piece, slot], scatter_recv.at[piece, slot],
            {"blk": block ^ (n_blk - 1 - slot)},
        )

    def scatter(piece, target, held_back):
        far = (block >= n_blk // 2) if n_blk // 4 <= target < n_blk // 2 else None
        if held_back:
            ready = far
        elif far is None:
            ready = block != target
        else:
            ready = jnp.logical_and(block != target, jnp.logical_not(far))

        @pl.when(ready)
        def _():
            scatter_copy(piece, (n_blk - 1) - (block ^ target)).start()

    def own_rows():
        value = contract(merged[:, side(mine)], last[mine])
        for slot in range(n_blk):
            for g in range(pieces):
                start = slot * owned + g * group
                part = value[start : start + group]
                partial[start : start + group, :] = pltpu.roll(part, g * width, 1) if g else part

    def other_rows(piece):
        value = last[1 - mine, spans[piece], :]
        return contract(merged[:, side(1 - mine)], jnp.concatenate([value] * pieces, axis=0))

    def weights(level, which):
        return transfer.at[level] if which else foreign.at[level - 1]

    def turn(level, inner):
        bit = bit_of(level)
        for half, which in ((0, bit), (1, 1 - bit)):
            turned[inner, half * rank : (half + 1) * rank] = weights(level, inner)[:, side(which)].T

    loads[0].wait()
    loads[1].wait()
    state = jnp.dot(column[...], ports[...], preferred_element_type=F32)
    first[core] = state.T.astype(BF16)
    pl.semaphore_wait(barrier, 1 + len(mixed_bits) + blk_bits + core * len(host_bits))
    tell(0)
    first_copy.start()
    for level in range(final):
        transfer_loads[level].wait()

    @pl.when(helper)
    def _():
        for copy in weight_copies:
            copy.start()

    own = contract(first[core], transfer[0, :, side(core)])
    transfer_loads[final].wait()
    for copy in row_loads:
        copy.wait()
    merged[...] = jnp.dot(row[...], transfer[final], preferred_element_type=F32).astype(BF16)

    @pl.when(host)
    def _():
        if len(stages[0]) == 2:
            turn(entry, 1)

    first_copy.wait_recv()
    state = own + contract(first[1 - core], transfer[0, :, side(1 - core)])
    held[0, core] = state.astype(BF16)
    for piece in range(pieces):
        stage_copy(0, core, piece).start()
    hear(0)
    tell(1)

    @pl.when(helper)
    def _():
        held_copy.start()
        for piece in range(pieces):
            down_copy(piece).wait_recv()
        own_rows()

    def mix(index, states, incoming_side):
        stage = stages[index]
        if len(stage) == 2:
            joined = jnp.concatenate(states, axis=1)
            return jnp.dot(joined, mixing[incoming_side], preferred_element_type=F32)
        which = bit_of(stage[0]) if incoming_side == 0 else 1 - bit_of(stage[0])
        return jnp.concatenate(
            [contract(states[c], weights(stage[0], c)[:, side(which)]) for c in range(2)], axis=1
        )

    def join(low, high, inner, outer):
        both = contract(turned[inner], weights(high, outer)[:, inner * rank : (inner + 1) * rank])
        for half in range(2):
            mixing[half, inner * rank : (inner + 1) * rank, outer * rank : (outer + 1) * rank] = both[
                half * rank : (half + 1) * rank
            ].astype(BF16)

    def prepare(stage):
        low, high = stage
        join(low, high, 1, 1)
        weight_copies[low - 1].wait_recv()
        turn(low, 0)
        join(low, high, 0, 1)
        weight_copies[high - 1].wait_recv()
        join(low, high, 1, 0)
        join(low, high, 0, 0)

    @pl.when(host)
    def _():
        for index, stage in enumerate(stages):
            if len(stage) == 2:
                if index:
                    turn(stage[0], 1)
                prepare(stage)
            else:
                weight_copies[stage[0] - 1].wait_recv()
            if index == 0:
                held_copy.wait_recv()
            begun[...] = mix(index, [held[index, 0], held[index, 1]], 0)
            for piece in range(pieces):
                for which in range(2):
                    stage_copy(index, which, piece).wait_recv()
                total = begun[spans[piece], :] + mix(
                    index, [arrived[index, 0, spans[piece], :], arrived[index, 1, spans[piece], :]], 1
                )
                total = total.astype(BF16)
                if index + 1 < len(stages):
                    for which in range(2):
                        held[index + 1, which, spans[piece], :] = total[:, which * rank : (which + 1) * rank]
                        stage_copy(index + 1, which, piece).start()
                else:
                    lent[spans[piece], :] = total[:, :rank]
                    last_copy(0, piece).start()
                    last[mine, spans[piece], :] = total[:, rank:]
                    last_copy(1, piece).start()
                    down_copy(piece).start()
        own_rows()

    for hop in range(1, blk_bits - 1):
        hear(hop)
        tell(hop + 1)
    lane = lax.broadcasted_iota(jnp.int32, (group, count), 1)

    def choose(values):
        result = values[0]
        for k in range(1, pieces):
            result = jnp.where(lane < k * width, result, values[k])
        return result

    for piece in range(pieces):
        last_copy(1, piece).wait_recv()
        total = partial[...] + other_rows(piece)
        for slot in range(n_blk):
            packed = choose(
                [
                    total[slot * owned + g * group : slot * owned + (g + 1) * group]
                    for g in ((k - piece) % pieces for k in range(pieces))
                ]
            )
            outgoing[piece, slot] = packed.astype(BF16)
        for target in range(n_blk):
            scatter(piece, target, False)
    for piece in range(pieces):
        for target in range(n_blk // 4, n_blk // 2):
            scatter(piece, target, True)

    first_copy.wait_send()
    for piece in range(pieces):
        stage_copy(0, core, piece).wait_send()

    @pl.when(helper)
    def _():
        held_copy.wait_send()
        for copy in weight_copies:
            copy.wait_send()

    @pl.when(host)
    def _():
        for piece in range(pieces):
            for index in range(1, len(stages)):
                for which in range(2):
                    stage_copy(index, which, piece).wait_send()
            last_copy(0, piece).wait_send()
            last_copy(1, piece).wait_send()
            down_copy(piece).wait_send()

    sums = []
    for piece in range(pieces):
        if piece == pieces - 1:
            for other in range(pieces):
                for slot in range(n_blk - 1):
                    scatter_copy(other, slot).wait_send()
        total = outgoing[piece, n_blk - 1].astype(F32)
        for slot in range(n_blk - 2, -1, -1):
            scatter_copy(piece, slot).wait_recv()
            total = total + incoming[piece, slot].astype(F32)
        sums.append(total * (1.0 / math.sqrt(n_blk)))
    for g in range(pieces):
        value = choose([sums[(k - g) % pieces] for k in range(pieces)])
        if g:
            value = pltpu.roll(value, (count - g * width) % count, 1)
        out_ref[0, g * group : (g + 1) * group, :] = value.astype(BF16)


def solution(mesh):
    n_blk, n_bfly = mesh.shape["blk"], mesh.shape["bfly"]

    def local(port_vectors, column_leaf, transfer, row_leaf):
        _, _, leaf, ports = port_vectors.shape
        rank = column_leaf.shape[2]
        levels = transfer.shape[1]
        rows = row_leaf.shape[2]
        owned = rows // n_blk
        _, stages = plan(levels, n_bfly.bit_length() - 1)
        assert n_blk & (n_blk - 1) == 0
        dma = pltpu.SemaphoreType.DMA
        return pl.pallas_call(
            functools.partial(kernel, n_blk, n_bfly, PIECES),
            out_shape=pltpu.VMEM((1, owned, ports), BF16),
            in_specs=[pl.BlockSpec(memory_space=pl.ANY)] * 4,
            out_specs=pl.BlockSpec(memory_space=pltpu.VMEM),
            scratch_shapes=[
                pltpu.VMEM((leaf, ports), BF16),
                pltpu.VMEM((rank, leaf), BF16),
                pltpu.VMEM((levels, rank, 2 * rank), BF16),
                pltpu.VMEM((levels - 2, rank, 2 * rank), BF16),
                pltpu.VMEM((rows, rank), BF16),
                pltpu.VMEM((2, ports, rank), BF16),
                pltpu.VMEM((len(stages), 2, ports, rank), BF16),
                pltpu.VMEM((len(stages), 2, ports, rank), BF16),
                pltpu.VMEM((ports, 2 * rank), F32),
                pltpu.VMEM((2, 2 * rank, rank), BF16),
                pltpu.VMEM((2, 2 * rank, 2 * rank), BF16),
                pltpu.VMEM((ports, rank), BF16),
                pltpu.VMEM((2, ports, rank), BF16),
                pltpu.VMEM((PIECES, n_blk, owned // PIECES, ports), BF16),
                pltpu.VMEM((PIECES, n_blk, owned // PIECES, ports), BF16),
                pltpu.VMEM((rows, 2 * rank), BF16),
                pltpu.VMEM((rows, ports), F32),
                dma((levels + 2,)),
                dma((n_blk,)),
                dma((2,)),
                dma((levels - 2,)),
                dma((levels - 2,)),
                dma((2,)),
                dma((len(stages), 2, PIECES)),
                dma((len(stages), 2, PIECES)),
                dma((2, PIECES)),
                dma((PIECES,)),
                dma((PIECES,)),
                dma((PIECES,)),
                dma((PIECES, n_blk)),
                dma((PIECES, n_blk)),
                pltpu.SemaphoreType.REGULAR((n_blk.bit_length(), n_blk.bit_length())),
            ],
            compiler_params=pltpu.CompilerParams(collective_id=0, has_side_effects=True),
        )(port_vectors, column_leaf, transfer, row_leaf)

    placed = (
        P("blk", "bfly", None, None),
        P("blk", "bfly", None, None),
        P("blk", None, "bfly", None, None),
        P("blk", "bfly", None, None),
    )
    return jax.shard_map(
        local, mesh=mesh, in_specs=placed, out_specs=P("bfly", "blk", None), check_vma=False
    )
```

```python
import functools
import math

import jax
import jax.numpy as jnp
from jax import lax
from jax.experimental import pallas as pl
from jax.experimental.pallas import tpu as pltpu
from jax.sharding import PartitionSpec as P

PIECES = 4
MESH = pl.DeviceIdType.MESH
F32 = jnp.float32
BF16 = jnp.bfloat16


def plan(levels, bit_count):
    bits = [level % bit_count for level in range(levels)]
    stages, level = [], 1
    while level < levels - 1:
        assert bits[level] > 0
        pair = level + 1 < levels - 1 and bits[level + 1] == 0
        stages.append((level, level + 1) if pair else (level,))
        level += len(stages[-1])
    assert stages and bits[levels - 1] > 0
    return bits, stages


def contract(left, right):
    return lax.dot_general(left, right, (((1,), (1,)), ((), ())), preferred_element_type=F32)


def kernel(
    n_blk, n_bfly, pieces,
    ports_hbm, column_hbm, transfer_hbm, row_hbm, out_ref,
    ports, column, transfer, foreign, row, first, held, arrived, begun, turned, mixing, lent,
    last, outgoing, incoming, merged, partial,
    load_sem, first_sem, weight_sem, held_sem, stage_send, stage_recv, last_send, last_recv, down_sem,
    scatter_send, scatter_recv, meet_sem,
):
    levels, rank, _ = transfer.shape
    count = ports.shape[1]
    leaf = row.shape[0]
    owned = leaf // n_blk
    bits, stages = plan(levels, n_bfly.bit_length() - 1)
    entry, final = stages[0][0], levels - 1
    block = lax.axis_index("blk")
    position = lax.axis_index("bfly")
    core = lax.rem(position, 2)
    host, helper = core == 1, core == 0
    width = count // pieces
    spans = [pl.ds(piece * width, width) for piece in range(pieces)]
    group = owned // pieces

    def load(source, target, sem):
        copy = pltpu.make_async_copy(source, target, sem)
        copy.start()
        return copy

    loads = [
        load(ports_hbm.at[0, 0], ports, load_sem.at[levels]),
        load(column_hbm.at[0, 0], column, load_sem.at[levels + 1]),
    ]
    transfer_loads = {
        level: load(transfer_hbm.at[0, level, 0], transfer.at[level], load_sem.at[level])
        for level in range(levels)
    }
    row_loads = []
    for slot in range(n_blk):
        owner = block ^ (n_blk - 1 - slot)
        row_loads.append(
            load(
                row_hbm.at[0, 0, pl.ds(pl.multiple_of(owner * owned, owned), owned)],
                row.at[pl.ds(slot * owned, owned)],
                load_sem.at[levels + 2],
            )
        )

    def side(which):
        return pl.ds(pl.multiple_of(which * rank, rank), rank)

    def bit_of(level):
        return lax.rem(position // 2 ** bits[level], 2)

    def across(level, to_core):
        place = position + (1 - 2 * bit_of(level)) * 2 ** bits[level]
        return {"bfly": place - core + to_core}

    mate = {"bfly": position + 1 - 2 * core}
    barrier = pltpu.get_barrier_semaphore()

    def greet(target):
        pl.semaphore_signal(barrier, inc=1, device_id=target, device_id_type=MESH)

    host_bits = {}
    for level in [stage[0] for stage in stages] + [final]:
        host_bits.setdefault(bits[level], level)
    mixed_bits = {bits[final]: final, bits[entry]: entry}
    greet(mate)
    for level in mixed_bits.values():
        greet(across(level, 1 - core))

    @pl.when(host)
    def _():
        for level in host_bits.values():
            greet(across(level, 1))

    blk_bits = n_blk.bit_length() - 1
    for bit in range(blk_bits):
        greet({"blk": block ^ (1 << bit)})

    def tell(turn):
        if turn < blk_bits - 1:
            for bit in range(blk_bits):
                pl.semaphore_signal(
                    meet_sem.at[turn], inc=1, device_id={"blk": block ^ (1 << bit)}, device_id_type=MESH
                )

    def hear(turn):
        if turn < blk_bits - 1:
            pl.semaphore_wait(meet_sem.at[turn], blk_bits)

    def remote(source, target, send_sem, recv_sem, device):
        return pltpu.make_async_remote_copy(
            src_ref=source, dst_ref=target, send_sem=send_sem, recv_sem=recv_sem,
            device_id=device, device_id_type=MESH,
        )

    first_copy = remote(first.at[core], first.at[core], first_sem.at[0], first_sem.at[1], mate)
    held_copy = remote(held.at[0, 0], held.at[0, 0], held_sem.at[0], held_sem.at[1], mate)

    def swap_copy(index):
        stage = stages[index]
        if len(stage) == 2:
            source, target = transfer.at[stage[1], :, side(1 - core)], foreign.at[index, :, pl.ds(0, rank)]
        else:
            source, target = transfer.at[stage[0]], foreign.at[index]
        return remote(source, target, weight_sem.at[index, 0], weight_sem.at[index, 1], mate)

    def mixing_copy(index, outer):
        part = mixing.at[index, :, pl.ds(0, rank), pl.ds(outer * rank, rank)]
        return remote(part, part, weight_sem.at[index, 2 + outer], weight_sem.at[index, 4 + outer], mate)

    def stage_start(index, which, piece):
        remote(
            held.at[index, which, spans[piece]], arrived.at[index, which, spans[piece]],
            stage_send.at[index], stage_recv.at[index, piece], across(stages[index][0], 1),
        ).start()

    def stage_arrival(index, piece):
        both = arrived.at[index, :, spans[piece]]
        return remote(both, both, stage_send.at[index], stage_recv.at[index, piece], mate)

    mine = bit_of(final)

    def last_copy(which, piece):
        source = lent.at[spans[piece]] if which == 0 else last.at[mine, spans[piece]]
        return remote(
            source, last.at[mine, spans[piece]], last_send.at[which], last_recv.at[piece], across(final, which)
        )

    def down_copy(span):
        return remote(lent.at[span], last.at[mine, span], down_sem.at[0], down_sem.at[1], mate)

    def scatter_copy(piece, slot):
        return remote(
            outgoing.at[piece, slot], incoming.at[piece, slot], scatter_send.at[0], scatter_recv.at[piece],
            {"blk": block ^ (n_blk - 1 - slot)},
        )

    everything, others = pl.ds(0, count), pl.ds(0, n_blk - 1)

    def scatter(piece, target, held_back):
        far = (block >= n_blk // 2) if n_blk // 4 <= target < n_blk // 2 else None
        if held_back:
            ready = far
        elif far is None:
            ready = block != target
        else:
            ready = jnp.logical_and(block != target, jnp.logical_not(far))

        @pl.when(ready)
        def _():
            scatter_copy(piece, (n_blk - 1) - (block ^ target)).start()

    def own_rows():
        value = contract(merged[:, side(mine)], last[mine])
        for slot in range(n_blk):
            for g in range(pieces):
                start = slot * owned + g * group
                part = value[start : start + group]
                partial[start : start + group, :] = pltpu.roll(part, g * width, 1) if g else part

    def other_rows(piece):
        value = last[1 - mine, spans[piece], :]
        return contract(merged[:, side(1 - mine)], jnp.concatenate([value] * pieces, axis=0))

    def turn(index):
        level = stages[index][0]
        bit = bit_of(level)
        for half, which in ((0, bit), (1, 1 - bit)):
            turned[half * rank : (half + 1) * rank] = transfer[level, :, side(which)].T

    def join(index, outer, factor):
        both = contract(turned[...], factor).astype(BF16)
        for half in range(2):
            mixing[index, half, side(core), side(outer)] = both[half * rank : (half + 1) * rank]

    loads[0].wait()
    loads[1].wait()
    state = jnp.dot(column[...], ports[...], preferred_element_type=F32)
    first[core] = state.T.astype(BF16)
    pl.semaphore_wait(barrier, 1 + len(mixed_bits) + blk_bits + core * len(host_bits))
    tell(0)
    first_copy.start()
    for level in range(final):
        transfer_loads[level].wait()
    for index, stage in enumerate(stages):
        if len(stage) == 2:
            swap_copy(index).start()
    own = contract(first[core], transfer[0, :, side(core)])
    if len(stages[0]) == 2:
        turn(0)
        join(0, core, transfer[stages[0][1], :, side(core)])
    first_copy.wait_recv()
    state = own + contract(first[1 - core], transfer[0, :, side(1 - core)])
    held[0, core] = state.astype(BF16)
    for piece in range(pieces):
        stage_start(0, core, piece)

    @pl.when(helper)
    def _():
        held_copy.start()
        for index, stage in enumerate(stages):
            if len(stage) == 1:
                swap_copy(index).start()
            elif index == 0:
                mixing_copy(index, 0).start()

    hear(0)
    tell(1)
    for index, stage in enumerate(stages):
        if len(stage) == 2:
            if index:
                turn(index)
                join(index, core, transfer[stage[1], :, side(core)])
            swap_copy(index).wait_recv()
            join(index, 1 - core, foreign[index, :, :rank])

            @pl.when(helper)
            def _():
                for outer in range(0 if index else 1, 2):
                    mixing_copy(index, outer).start()

    transfer_loads[final].wait()
    whole = pltpu.make_async_copy(row, row, load_sem.at[levels + 2])
    whole.wait()
    merged[...] = jnp.dot(row[...], transfer[final], preferred_element_type=F32).astype(BF16)

    @pl.when(helper)
    def _():
        down_copy(everything).wait_recv()

    def mix(index, states, arriving):
        stage = stages[index]
        if len(stage) == 2:
            return jnp.dot(jnp.concatenate(states, axis=1), mixing[index, arriving], preferred_element_type=F32)
        bit = bit_of(stage[0])
        which = side(1 - bit if arriving else bit)
        factors = [foreign[index, :, which], transfer[stage[0], :, which]]
        return jnp.concatenate([contract(*pair) for pair in zip(states, factors)], axis=1)

    @pl.when(host)
    def _():
        held_copy.wait_recv()
        for index, stage in enumerate(stages):
            if len(stage) == 2:
                mixing_copy(index, 0).wait_recv()
                mixing_copy(index, 1).wait_recv()
            else:
                swap_copy(index).wait_recv()
            begun[...] = mix(index, [held[index, 0], held[index, 1]], 0)
            for piece in range(pieces):
                stage_arrival(index, piece).wait_recv()
                total = begun[spans[piece], :] + mix(
                    index, [arrived[index, 0, spans[piece], :], arrived[index, 1, spans[piece], :]], 1
                )
                total = total.astype(BF16)
                if index + 1 < len(stages):
                    for which in range(2):
                        held[index + 1, which, spans[piece], :] = total[:, which * rank : (which + 1) * rank]
                        stage_start(index + 1, which, piece)
                else:
                    lent[spans[piece], :] = total[:, :rank]
                    last_copy(0, piece).start()
                    last[mine, spans[piece], :] = total[:, rank:]
                    last_copy(1, piece).start()
                    down_copy(spans[piece]).start()

    own_rows()
    for hop in range(1, blk_bits - 1):
        hear(hop)
        tell(hop + 1)
    lane = lax.broadcasted_iota(jnp.int32, (group, count), 1)

    def choose(values):
        result = values[0]
        for k in range(1, pieces):
            result = jnp.where(lane < k * width, result, values[k])
        return result

    for piece in range(pieces):
        last_copy(1, piece).wait_recv()
        total = partial[...] + other_rows(piece)
        for slot in range(n_blk):
            packed = choose(
                [
                    total[slot * owned + g * group : slot * owned + (g + 1) * group]
                    for g in ((k - piece) % pieces for k in range(pieces))
                ]
            )
            outgoing[piece, slot] = packed.astype(BF16)
        for target in range(n_blk):
            scatter(piece, target, False)
    for piece in range(pieces):
        for target in range(n_blk // 4, n_blk // 2):
            scatter(piece, target, True)

    def sent(index, which):
        source = held.at[index, which] if index == 0 else held.at[index]
        remote(source, source, stage_send.at[index], stage_recv.at[index, 0], mate).wait_send()

    first_copy.wait_send()
    sent(0, core)
    for index, stage in enumerate(stages):
        if len(stage) == 2:
            swap_copy(index).wait_send()

    @pl.when(helper)
    def _():
        held_copy.wait_send()
        for index, stage in enumerate(stages):
            if len(stage) == 1:
                swap_copy(index).wait_send()
            else:
                mixing_copy(index, 0).wait_send()
                mixing_copy(index, 1).wait_send()

    @pl.when(host)
    def _():
        for index in range(1, len(stages)):
            sent(index, 0)
        for which in range(2):
            whole = last.at[mine]
            remote(whole, whole, last_send.at[which], last_recv.at[0], mate).wait_send()
        down_copy(everything).wait_send()

    sums = []
    for piece in range(pieces):
        if piece == pieces - 1:
            whole = outgoing.at[:, others]
            remote(whole, whole, scatter_send.at[0], scatter_recv.at[0], mate).wait_send()
        whole = incoming.at[piece, others]
        remote(whole, whole, scatter_send.at[0], scatter_recv.at[piece], mate).wait_recv()
        total = outgoing[piece, n_blk - 1].astype(F32)
        for slot in range(n_blk - 2, -1, -1):
            total = total + incoming[piece, slot].astype(F32)
        sums.append(total * (1.0 / math.sqrt(n_blk)))
    for g in range(pieces):
        value = choose([sums[(k - g) % pieces] for k in range(pieces)])
        if g:
            value = pltpu.roll(value, (count - g * width) % count, 1)
        out_ref[0, g * group : (g + 1) * group, :] = value.astype(BF16)


def solution(mesh):
    n_blk, n_bfly = mesh.shape["blk"], mesh.shape["bfly"]

    def local(port_vectors, column_leaf, transfer, row_leaf):
        _, _, leaf, ports = port_vectors.shape
        rank = column_leaf.shape[2]
        levels = transfer.shape[1]
        rows = row_leaf.shape[2]
        owned = rows // n_blk
        depth = len(plan(levels, n_bfly.bit_length() - 1)[1])
        assert n_blk & (n_blk - 1) == 0
        dma = pltpu.SemaphoreType.DMA
        return pl.pallas_call(
            functools.partial(kernel, n_blk, n_bfly, PIECES),
            out_shape=pltpu.VMEM((1, owned, ports), BF16),
            in_specs=[pl.BlockSpec(memory_space=pl.ANY)] * 4,
            out_specs=pl.BlockSpec(memory_space=pltpu.VMEM),
            scratch_shapes=[
                pltpu.VMEM((leaf, ports), BF16),
                pltpu.VMEM((rank, leaf), BF16),
                pltpu.VMEM((levels, rank, 2 * rank), BF16),
                pltpu.VMEM((depth, rank, 2 * rank), BF16),
                pltpu.VMEM((rows, rank), BF16),
                pltpu.VMEM((2, ports, rank), BF16),
                pltpu.VMEM((depth, 2, ports, rank), BF16),
                pltpu.VMEM((depth, 2, ports, rank), BF16),
                pltpu.VMEM((ports, 2 * rank), F32),
                pltpu.VMEM((2 * rank, rank), BF16),
                pltpu.VMEM((depth, 2, 2 * rank, 2 * rank), BF16),
                pltpu.VMEM((ports, rank), BF16),
                pltpu.VMEM((2, ports, rank), BF16),
                pltpu.VMEM((PIECES, n_blk, owned // PIECES, ports), BF16),
                pltpu.VMEM((PIECES, n_blk, owned // PIECES, ports), BF16),
                pltpu.VMEM((rows, 2 * rank), BF16),
                pltpu.VMEM((rows, ports), F32),
                dma((levels + 3,)),
                dma((2,)),
                dma((depth, 6)),
                dma((2,)),
                dma((depth,)),
                dma((depth, PIECES)),
                dma((2,)),
                dma((PIECES,)),
                dma((2,)),
                dma((1,)),
                dma((PIECES,)),
                pltpu.SemaphoreType.REGULAR((max(1, n_blk.bit_length() - 2),)),
            ],
            compiler_params=pltpu.CompilerParams(collective_id=0, has_side_effects=True),
        )(port_vectors, column_leaf, transfer, row_leaf)

    placed = (
        P("blk", "bfly", None, None),
        P("blk", "bfly", None, None),
        P("blk", None, "bfly", None, None),
        P("blk", "bfly", None, None),
    )
    return jax.shard_map(
        local, mesh=mesh, in_specs=placed, out_specs=P("bfly", "blk", None), check_vma=False
    )
```

```python
import functools
import math

import jax
import jax.numpy as jnp
from jax import lax
from jax.experimental import pallas as pl
from jax.experimental.pallas import tpu as pltpu
from jax.sharding import PartitionSpec as P

PIECES = 4
GROUPS = 2
MESH = pl.DeviceIdType.MESH
F32 = jnp.float32
BF16 = jnp.bfloat16


def plan(levels, bit_count):
    bits = [level % bit_count for level in range(levels)]
    stages, level = [], 1
    while level < levels - 1:
        assert bits[level] > 0
        pair = level + 1 < levels - 1 and bits[level + 1] == 0
        stages.append((level, level + 1) if pair else (level,))
        level += len(stages[-1])
    assert stages and bits[levels - 1] > 0
    return bits, stages


def contract(left, right):
    return lax.dot_general(left, right, (((1,), (1,)), ((), ())), preferred_element_type=F32)


def kernel(
    n_blk, n_bfly, pieces, groups,
    ports_hbm, column_hbm, transfer_hbm, row_hbm, out_ref,
    ports, column, transfer, foreign, upper, row, first, held, arrived, begun, turned, mixing, lent,
    last, outgoing, incoming, merged, partial,
    load_sem, first_sem, weight_sem, held_sem, stage_send, stage_recv, last_send, last_recv, down_sem,
    scatter_send, scatter_recv, meet_sem,
):
    levels, rank, _ = transfer.shape
    count = ports.shape[1]
    leaf = row.shape[0]
    owned = leaf // n_blk
    bits, stages = plan(levels, n_bfly.bit_length() - 1)
    entry, final = stages[0][0], levels - 1
    block = lax.axis_index("blk")
    position = lax.axis_index("bfly")
    core = lax.rem(position, 2)
    host, helper = core == 1, core == 0
    width = count // pieces
    spans = [pl.ds(piece * width, width) for piece in range(pieces)]
    tall, wide, quarter = owned // groups, count // groups, n_blk // 4

    def load(source, target, sem):
        copy = pltpu.make_async_copy(source, target, sem)
        copy.start()
        return copy

    loads = [
        load(ports_hbm.at[0, 0], ports, load_sem.at[levels]),
        load(column_hbm.at[0, 0], column, load_sem.at[levels + 1]),
    ]
    transfer_loads = {
        level: load(transfer_hbm.at[0, level, 0], transfer.at[level], load_sem.at[level])
        for level in range(levels)
    }
    row_load = load(row_hbm.at[0, 0], row, load_sem.at[levels + 2])

    def side(which):
        return pl.ds(pl.multiple_of(which * rank, rank), rank)

    def bit_of(level):
        return lax.rem(position // 2 ** bits[level], 2)

    def across(level, to_core):
        place = position + (1 - 2 * bit_of(level)) * 2 ** bits[level]
        return {"bfly": place - core + to_core}

    def near_peers(distance):
        pair = block // 2
        return [
            (pair >= 0, {"blk": block + 1 - 2 * lax.rem(block, 2)}),
            (pair >= distance, {"blk": block - 2 * distance}),
            (pair + distance < n_blk // 2, {"blk": block + 2 * distance}),
        ]

    def number(peers):
        return sum(there.astype(jnp.int32) for there, _ in peers)

    mate = {"bfly": position + 1 - 2 * core}
    barrier = pltpu.get_barrier_semaphore()

    def greet(target):
        pl.semaphore_signal(barrier, inc=1, device_id=target, device_id_type=MESH)

    host_bits = {}
    for level in [stage[0] for stage in stages] + [final]:
        host_bits.setdefault(bits[level], level)
    mixed_bits = {bits[final]: final, bits[entry]: entry}
    greet(mate)
    for level in mixed_bits.values():
        greet(across(level, 1 - core))

    @pl.when(host)
    def _():
        for level in host_bits.values():
            greet(across(level, 1))

    near = near_peers(1)
    for there, peer in near:
        pl.when(there)(functools.partial(greet, peer))

    turns = (n_blk // 2).bit_length() - 1

    def tell(turn):
        if turn < turns:
            for there, peer in near_peers(2**turn):

                @pl.when(there)
                def _(peer=peer):
                    pl.semaphore_signal(meet_sem.at[turn], inc=1, device_id=peer, device_id_type=MESH)

    def hear(turn):
        if turn < turns:
            pl.semaphore_wait(meet_sem.at[turn], number(near_peers(2**turn)))

    def remote(source, target, send_sem, recv_sem, device):
        return pltpu.make_async_remote_copy(
            src_ref=source, dst_ref=target, send_sem=send_sem, recv_sem=recv_sem,
            device_id=device, device_id_type=MESH,
        )

    first_copy = remote(first.at[core], first.at[core], first_sem.at[0], first_sem.at[1], mate)
    held_copy = remote(held.at[0, 0], held.at[0, 0], held_sem.at[0], held_sem.at[1], mate)

    def lower_copy(index):
        return remote(
            transfer.at[stages[index][0]], foreign.at[index], weight_sem.at[index, 0], weight_sem.at[index, 1], mate
        )

    def upper_copy(index):
        return remote(
            transfer.at[stages[index][1], :, pl.ds(rank, rank)], upper.at[index], weight_sem.at[index, 2],
            weight_sem.at[index, 3], mate,
        )

    def mixing_copy(index, half):
        part = mixing.at[index, half, pl.ds(0, rank), pl.ds(0, rank)]
        return remote(part, part, weight_sem.at[index, 4], weight_sem.at[index, 5 + half], mate)

    def stage_start(index, which, piece):
        remote(
            held.at[index, which, spans[piece]], arrived.at[index, which, spans[piece]],
            stage_send.at[index], stage_recv.at[index, piece], across(stages[index][0], 1),
        ).start()

    def stage_arrival(index, piece):
        both = arrived.at[index, :, spans[piece]]
        return remote(both, both, stage_send.at[index], stage_recv.at[index, piece], mate)

    mine = bit_of(final)

    def last_copy(which, piece):
        source = lent.at[spans[piece]] if which == 0 else last.at[mine, spans[piece]]
        return remote(
            source, last.at[mine, spans[piece]], last_send.at[which], last_recv.at[piece], across(final, which)
        )

    def down_copy(span):
        return remote(lent.at[span], last.at[mine, span], down_sem.at[0], down_sem.at[1], mate)

    everything, others = pl.ds(0, count), pl.ds(0, n_blk - 1)

    def scatter(part, target, late):
        ready = block != target
        if target >= quarter:
            far = block >= n_blk - quarter
            ready = jnp.logical_and(ready, far if late else jnp.logical_not(far))
        elif late:
            return

        @pl.when(ready)
        def _():
            remote(
                outgoing.at[part, target], incoming.at[part, block], scatter_send.at[0], scatter_recv.at[part],
                {"blk": target},
            ).start()

    def own_rows():
        value = contract(merged[:, side(mine)], last[mine])
        for start in range(0, leaf, tall):
            shift = start // tall % groups * wide
            rows = value[start : start + tall]
            partial[start : start + tall, :] = pltpu.roll(rows, shift, 1) if shift else rows

    def other_rows(part, first_row, end_row):
        value = last[1 - mine, part * wide : (part + 1) * wide, :]
        return contract(merged[first_row:end_row, side(1 - mine)], jnp.concatenate([value] * groups, axis=0))

    def turn(index, slot, matrix):
        bit = bit_of(stages[index][0])
        for half, which in ((0, bit), (1, 1 - bit)):
            turned[slot, half * rank : (half + 1) * rank] = matrix[:, side(which)].T

    def join(index, slot, inner, outer, factor):
        both = contract(turned[slot], factor).astype(BF16)
        for half in range(2):
            mixing[index, half, side(inner), side(outer)] = both[half * rank : (half + 1) * rank]

    def join_own(index):
        low, high = stages[index]
        turn(index, 0, transfer.at[low])
        join(index, 0, core, core, transfer[high, :, side(core)])

    def merge_rows():
        transfer_loads[final].wait()
        row_load.wait()
        merged[...] = jnp.dot(row[...], transfer[final], preferred_element_type=F32).astype(BF16)

    loads[0].wait()
    loads[1].wait()
    state = jnp.dot(column[...], ports[...], preferred_element_type=F32)
    first[core] = state.T.astype(BF16)
    pl.semaphore_wait(barrier, 1 + len(mixed_bits) + core * len(host_bits) + number(near))
    tell(0)
    first_copy.start()
    for level in range(final):
        transfer_loads[level].wait()

    @pl.when(helper)
    def _():
        lower_copy(0).start()

    own = contract(first[core], transfer[0, :, side(core)])
    if len(stages[0]) == 2:
        join_own(0)
    first_copy.wait_recv()
    state = own + contract(first[1 - core], transfer[0, :, side(1 - core)])
    held[0, core] = state.astype(BF16)
    for piece in range(pieces):
        stage_start(0, core, piece)
    @pl.when(helper)
    def _():
        held_copy.start()
        for index, stage in enumerate(stages):
            if index:
                lower_copy(index).start()
            if len(stage) == 2:
                upper_copy(index).start()
                if index:
                    join_own(index)
                for half in range(2):
                    mixing_copy(index, half).start()

    def mix(index, states, arriving):
        stage = stages[index]
        if len(stage) == 2:
            return jnp.dot(jnp.concatenate(states, axis=1), mixing[index, arriving], preferred_element_type=F32)
        bit = bit_of(stage[0])
        which = side(1 - bit if arriving else bit)
        factors = [foreign[index, :, which], transfer[stage[0], :, which]]
        return jnp.concatenate([contract(*pair) for pair in zip(states, factors)], axis=1)

    @pl.when(host)
    def _():
        for index, stage in enumerate(stages):
            if len(stage) == 2:
                if index:
                    join_own(index)
                lower_copy(index).wait_recv()
                turn(index, 1, foreign.at[index])
                join(index, 1, 0, 1, transfer[stage[1], :, :rank])
                upper_copy(index).wait_recv()
                join(index, 0, 1, 0, upper[index])
                mixing_copy(index, 0).wait_recv()
            else:
                lower_copy(index).wait_recv()
            if index == 0:
                held_copy.wait_recv()
            begun[...] = mix(index, [held[index, 0], held[index, 1]], 0)
            if index == 0:
                hear(0)
                tell(1)
            if len(stage) == 2:
                mixing_copy(index, 1).wait_recv()
            for piece in range(pieces):
                stage_arrival(index, piece).wait_recv()
                total = begun[spans[piece], :] + mix(
                    index, [arrived[index, 0, spans[piece], :], arrived[index, 1, spans[piece], :]], 1
                )
                total = total.astype(BF16)
                if index + 1 < len(stages):
                    for which in range(2):
                        held[index + 1, which, spans[piece], :] = total[:, which * rank : (which + 1) * rank]
                        stage_start(index + 1, which, piece)
                else:
                    lent[spans[piece], :] = total[:, :rank]
                    last_copy(0, piece).start()
                    last[mine, spans[piece], :] = total[:, rank:]
                    last_copy(1, piece).start()
                    down_copy(spans[piece]).start()


    @pl.when(helper)
    def _():
        merge_rows()
        hear(0)
        tell(1)
        down_copy(everything).wait_recv()

    @pl.when(host)
    def _():
        merge_rows()

    own_rows()

    for hop in range(1, turns):
        hear(hop)
        tell(hop + 1)
    lane = lax.broadcasted_iota(jnp.int32, (tall, count), 1)

    def choose(values):
        result = values[0]
        for k in range(1, groups):
            result = jnp.where(lane < k * wide, result, values[k])
        return result

    for part in range(groups):
        for piece in range(part * pieces // groups, (part + 1) * pieces // groups):
            last_copy(1, piece).wait_recv()
        for low, high in ((0, quarter), (quarter, n_blk)):
            total = partial[low * owned : high * owned, :] + other_rows(part, low * owned, high * owned)
            for target in range(low, high):
                top = (target - low) * owned
                packed = choose(
                    [
                        total[top + g * tall : top + (g + 1) * tall]
                        for g in ((k - part) % groups for k in range(groups))
                    ]
                )
                outgoing[part, target] = packed.astype(BF16)
                scatter(part, target, False)
        incoming[part, block] = outgoing[part, block]
    for part in range(groups):
        for target in range(quarter, n_blk):
            scatter(part, target, True)

    def sent(index, which):
        source = held.at[index, which] if index == 0 else held.at[index]
        remote(source, source, stage_send.at[index], stage_recv.at[index, 0], mate).wait_send()

    first_copy.wait_send()
    sent(0, core)

    @pl.when(helper)
    def _():
        held_copy.wait_send()
        for index, stage in enumerate(stages):
            lower_copy(index).wait_send()
            if len(stage) == 2:
                upper_copy(index).wait_send()
                part = mixing.at[index, :, pl.ds(0, rank), pl.ds(0, rank)]
                remote(part, part, weight_sem.at[index, 4], weight_sem.at[index, 5], mate).wait_send()

    @pl.when(host)
    def _():
        for index in range(1, len(stages)):
            sent(index, 0)
        for which in range(2):
            whole = last.at[mine]
            remote(whole, whole, last_send.at[which], last_recv.at[0], mate).wait_send()
        down_copy(everything).wait_send()

    sums = []
    for part in range(groups):
        if part == groups - 1:
            whole = outgoing.at[:, others]
            remote(whole, whole, scatter_send.at[0], scatter_recv.at[0], mate).wait_send()
        whole = incoming.at[part, others]
        remote(whole, whole, scatter_send.at[0], scatter_recv.at[part], mate).wait_recv()
        total = incoming[part, 0].astype(F32)
        for source in range(1, n_blk):
            total = total + incoming[part, source].astype(F32)
        sums.append(total * (1.0 / math.sqrt(n_blk)))
    for g in range(groups):
        value = choose([sums[(k - g) % groups] for k in range(groups)])
        if g:
            value = pltpu.roll(value, (count - g * wide) % count, 1)
        out_ref[0, g * tall : (g + 1) * tall, :] = value.astype(BF16)


def solution(mesh):
    n_blk, n_bfly = mesh.shape["blk"], mesh.shape["bfly"]

    def local(port_vectors, column_leaf, transfer, row_leaf):
        _, _, leaf, ports = port_vectors.shape
        rank = column_leaf.shape[2]
        levels = transfer.shape[1]
        rows = row_leaf.shape[2]
        owned = rows // n_blk
        depth = len(plan(levels, n_bfly.bit_length() - 1)[1])
        assert n_blk % 4 == 0 and n_blk & (n_blk - 1) == 0
        dma = pltpu.SemaphoreType.DMA
        return pl.pallas_call(
            functools.partial(kernel, n_blk, n_bfly, PIECES, GROUPS),
            out_shape=pltpu.VMEM((1, owned, ports), BF16),
            in_specs=[pl.BlockSpec(memory_space=pl.ANY)] * 4,
            out_specs=pl.BlockSpec(memory_space=pltpu.VMEM),
            scratch_shapes=[
                pltpu.VMEM((leaf, ports), BF16),
                pltpu.VMEM((rank, leaf), BF16),
                pltpu.VMEM((levels, rank, 2 * rank), BF16),
                pltpu.VMEM((depth, rank, 2 * rank), BF16),
                pltpu.VMEM((depth, rank, rank), BF16),
                pltpu.VMEM((rows, rank), BF16),
                pltpu.VMEM((2, ports, rank), BF16),
                pltpu.VMEM((depth, 2, ports, rank), BF16),
                pltpu.VMEM((depth, 2, ports, rank), BF16),
                pltpu.VMEM((ports, 2 * rank), F32),
                pltpu.VMEM((2, 2 * rank, rank), BF16),
                pltpu.VMEM((depth, 2, 2 * rank, 2 * rank), BF16),
                pltpu.VMEM((ports, rank), BF16),
                pltpu.VMEM((2, ports, rank), BF16),
                pltpu.VMEM((GROUPS, n_blk, owned // GROUPS, ports), BF16),
                pltpu.VMEM((GROUPS, n_blk, owned // GROUPS, ports), BF16),
                pltpu.VMEM((rows, 2 * rank), BF16),
                pltpu.VMEM((rows, ports), F32),
                dma((levels + 3,)),
                dma((2,)),
                dma((depth, 7)),
                dma((2,)),
                dma((depth,)),
                dma((depth, PIECES)),
                dma((2,)),
                dma((PIECES,)),
                dma((2,)),
                dma((1,)),
                dma((GROUPS,)),
                pltpu.SemaphoreType.REGULAR((n_blk.bit_length(),)),
            ],
            compiler_params=pltpu.CompilerParams(collective_id=0, has_side_effects=True),
        )(port_vectors, column_leaf, transfer, row_leaf)

    placed = (
        P("blk", "bfly", None, None),
        P("blk", "bfly", None, None),
        P("blk", None, "bfly", None, None),
        P("blk", "bfly", None, None),
    )
    return jax.shard_map(
        local, mesh=mesh, in_specs=placed, out_specs=P("bfly", "blk", None), check_vma=False
    )
```

```python
import functools
import math

import jax
import jax.numpy as jnp
from jax import lax
from jax.experimental import pallas as pl
from jax.experimental.pallas import tpu as pltpu
from jax.sharding import PartitionSpec as P

PIECES = 4
GROUPS = 2
MESH = pl.DeviceIdType.MESH
F32 = jnp.float32
BF16 = jnp.bfloat16


def plan(levels, bit_count):
    bits = [level % bit_count for level in range(levels)]
    stages, level = [], 1
    while level < levels - 1:
        assert bits[level] > 0
        pair = level + 1 < levels - 1 and bits[level + 1] == 0
        stages.append((level, level + 1) if pair else (level,))
        level += len(stages[-1])
    assert stages and bits[levels - 1] > 0
    return bits, stages


def contract(left, right):
    return lax.dot_general(left, right, (((1,), (1,)), ((), ())), preferred_element_type=F32)


def kernel(
    n_blk, n_bfly, pieces, groups,
    ports_hbm, column_hbm, transfer_hbm, row_hbm, out_ref,
    ports, column, transfer, foreign, upper, row, first, held, arrived, begun, turned, mixing, lent,
    last, outgoing, incoming, merged, partial,
    load_sem, first_sem, weight_sem, held_sem, stage_send, stage_recv, last_send, last_recv, down_sem,
    scatter_send, scatter_recv, meet_sem,
):
    levels, rank, _ = transfer.shape
    count = ports.shape[1]
    leaf = row.shape[0]
    owned = leaf // n_blk
    bits, stages = plan(levels, n_bfly.bit_length() - 1)
    entry, final = stages[0][0], levels - 1
    block = lax.axis_index("blk")
    position = lax.axis_index("bfly")
    core = lax.rem(position, 2)
    host, helper = core == 1, core == 0
    width = count // pieces
    spans = [pl.ds(piece * width, width) for piece in range(pieces)]
    tall, wide, quarter = owned // groups, count // groups, n_blk // 4

    def load(source, target, sem):
        copy = pltpu.make_async_copy(source, target, sem)
        copy.start()
        return copy

    loads = [
        load(ports_hbm.at[0, 0], ports, load_sem.at[levels]),
        load(column_hbm.at[0, 0], column, load_sem.at[levels + 1]),
    ]
    transfer_loads = {
        level: load(transfer_hbm.at[0, level, 0], transfer.at[level], load_sem.at[level])
        for level in range(levels)
    }
    row_load = load(row_hbm.at[0, 0], row, load_sem.at[levels + 2])

    def side(which):
        return pl.ds(pl.multiple_of(which * rank, rank), rank)

    def bit_of(level):
        return lax.rem(position // 2 ** bits[level], 2)

    def across(level, to_core):
        place = position + (1 - 2 * bit_of(level)) * 2 ** bits[level]
        return {"bfly": place - core + to_core}

    def near_peers(distance):
        pair = block // 2
        return [
            (pair >= 0, {"blk": block + 1 - 2 * lax.rem(block, 2)}),
            (pair >= distance, {"blk": block - 2 * distance}),
            (pair + distance < n_blk // 2, {"blk": block + 2 * distance}),
        ]

    def number(peers):
        return sum(there.astype(jnp.int32) for there, _ in peers)

    mate = {"bfly": position + 1 - 2 * core}
    barrier = pltpu.get_barrier_semaphore()

    def greet(target):
        pl.semaphore_signal(barrier, inc=1, device_id=target, device_id_type=MESH)

    host_bits = {}
    for level in [stage[0] for stage in stages] + [final]:
        host_bits.setdefault(bits[level], level)
    mixed_bits = {bits[final]: final, bits[entry]: entry}
    greet(mate)
    for level in mixed_bits.values():
        greet(across(level, 1 - core))

    @pl.when(host)
    def _():
        for level in host_bits.values():
            greet(across(level, 1))

    near = near_peers(1)
    for there, peer in near:
        pl.when(there)(functools.partial(greet, peer))

    turns = (n_blk // 2).bit_length() - 1

    def tell(turn):
        if turn < turns:
            for there, peer in near_peers(2**turn):

                @pl.when(there)
                def _(peer=peer):
                    pl.semaphore_signal(meet_sem.at[turn], inc=1, device_id=peer, device_id_type=MESH)

    def hear(turn):
        if turn < turns:
            pl.semaphore_wait(meet_sem.at[turn], number(near_peers(2**turn)))

    def remote(source, target, send_sem, recv_sem, device):
        return pltpu.make_async_remote_copy(
            src_ref=source, dst_ref=target, send_sem=send_sem, recv_sem=recv_sem,
            device_id=device, device_id_type=MESH,
        )

    first_copy = remote(first.at[core], first.at[core], first_sem.at[0], first_sem.at[1], mate)
    held_copy = remote(held.at[0, 0], held.at[0, 0], held_sem.at[0], held_sem.at[1], mate)

    def lower_copy(index):
        return remote(
            transfer.at[stages[index][0]], foreign.at[index], weight_sem.at[index, 0], weight_sem.at[index, 1], mate
        )

    def upper_copy(index):
        return remote(
            transfer.at[stages[index][1], :, pl.ds(rank, rank)], upper.at[index], weight_sem.at[index, 2],
            weight_sem.at[index, 3], mate,
        )

    def mixing_copy(index, half):
        part = mixing.at[index, half, pl.ds(0, rank), pl.ds(0, rank)]
        return remote(part, part, weight_sem.at[index, 4], weight_sem.at[index, 5 + half], mate)

    def stage_start(index, which, piece):
        remote(
            held.at[index, which, spans[piece]], arrived.at[index, which, spans[piece]],
            stage_send.at[index], stage_recv.at[index, piece], across(stages[index][0], 1),
        ).start()

    def stage_arrival(index, piece):
        both = arrived.at[index, :, spans[piece]]
        return remote(both, both, stage_send.at[index], stage_recv.at[index, piece], mate)

    mine = bit_of(final)

    def last_copy(which, piece):
        source = lent.at[spans[piece]] if which == 0 else last.at[mine, spans[piece]]
        return remote(
            source, last.at[mine, spans[piece]], last_send.at[which], last_recv.at[piece], across(final, which)
        )

    def down_copy(span):
        return remote(lent.at[span], last.at[mine, span], down_sem.at[0], down_sem.at[1], mate)

    everything, others = pl.ds(0, count), pl.ds(0, n_blk - 1)

    def scatter(part, target, late):
        ready = block != target
        if target >= quarter:
            far = block >= quarter
            ready = jnp.logical_and(ready, far if late else jnp.logical_not(far))
        elif late:
            return

        @pl.when(ready)
        def _():
            remote(
                outgoing.at[part, target], incoming.at[part, block], scatter_send.at[0], scatter_recv.at[part],
                {"blk": target},
            ).start()

    def own_rows():
        value = contract(merged[:, side(mine)], last[mine])
        for start in range(0, leaf, tall):
            shift = start // tall % groups * wide
            rows = value[start : start + tall]
            partial[start : start + tall, :] = pltpu.roll(rows, shift, 1) if shift else rows

    def other_rows(part, first_row, end_row):
        value = last[1 - mine, part * wide : (part + 1) * wide, :]
        return contract(merged[first_row:end_row, side(1 - mine)], jnp.concatenate([value] * groups, axis=0))

    def turn(index, slot, matrix):
        bit = bit_of(stages[index][0])
        for half, which in ((0, bit), (1, 1 - bit)):
            turned[slot, half * rank : (half + 1) * rank] = matrix[:, side(which)].T

    def join(index, slot, inner, outer, factor):
        both = contract(turned[slot], factor).astype(BF16)
        for half in range(2):
            mixing[index, half, side(inner), side(outer)] = both[half * rank : (half + 1) * rank]

    def join_own(index):
        low, high = stages[index]
        turn(index, 0, transfer.at[low])
        join(index, 0, core, core, transfer[high, :, side(core)])

    def merge_rows():
        transfer_loads[final].wait()
        row_load.wait()
        merged[...] = jnp.dot(row[...], transfer[final], preferred_element_type=F32).astype(BF16)

    loads[0].wait()
    loads[1].wait()
    state = lax.dot_general(ports[...], column[...], (((0,), (1,)), ((), ())), preferred_element_type=F32)
    first[core] = state.astype(BF16)
    pl.semaphore_wait(barrier, 1 + len(mixed_bits) + core * len(host_bits) + number(near))
    tell(0)
    first_copy.start()
    for level in range(final):
        transfer_loads[level].wait()

    @pl.when(helper)
    def _():
        lower_copy(0).start()

    own = contract(first[core], transfer[0, :, side(core)])
    if len(stages[0]) == 2:
        join_own(0)
    first_copy.wait_recv()
    state = own + contract(first[1 - core], transfer[0, :, side(1 - core)])
    held[0, core] = state.astype(BF16)
    for piece in range(pieces):
        stage_start(0, core, piece)
    @pl.when(helper)
    def _():
        held_copy.start()
        for index, stage in enumerate(stages):
            if index:
                lower_copy(index).start()
            if len(stage) == 2:
                upper_copy(index).start()
                if index:
                    join_own(index)
                for half in range(2):
                    mixing_copy(index, half).start()

    def mix(index, states, arriving):
        stage = stages[index]
        if len(stage) == 2:
            return jnp.dot(jnp.concatenate(states, axis=1), mixing[index, arriving], preferred_element_type=F32)
        bit = bit_of(stage[0])
        which = side(1 - bit if arriving else bit)
        factors = [foreign[index, :, which], transfer[stage[0], :, which]]
        return jnp.concatenate([contract(*pair) for pair in zip(states, factors)], axis=1)

    @pl.when(host)
    def _():
        for index, stage in enumerate(stages):
            if len(stage) == 2:
                if index:
                    join_own(index)
                lower_copy(index).wait_recv()
                turn(index, 1, foreign.at[index])
                join(index, 1, 0, 1, transfer[stage[1], :, :rank])
                upper_copy(index).wait_recv()
                join(index, 0, 1, 0, upper[index])
                mixing_copy(index, 0).wait_recv()
            else:
                lower_copy(index).wait_recv()
            if index == 0:
                held_copy.wait_recv()
            begun[...] = mix(index, [held[index, 0], held[index, 1]], 0)
            if index == 0:
                hear(0)
                tell(1)
            if len(stage) == 2:
                mixing_copy(index, 1).wait_recv()
            for piece in range(pieces):
                stage_arrival(index, piece).wait_recv()
                total = begun[spans[piece], :] + mix(
                    index, [arrived[index, 0, spans[piece], :], arrived[index, 1, spans[piece], :]], 1
                )
                total = total.astype(BF16)
                if index + 1 < len(stages):
                    for which in range(2):
                        held[index + 1, which, spans[piece], :] = total[:, which * rank : (which + 1) * rank]
                        stage_start(index + 1, which, piece)
                else:
                    lent[spans[piece], :] = total[:, :rank]
                    last_copy(0, piece).start()
                    last[mine, spans[piece], :] = total[:, rank:]
                    down_copy(spans[piece]).start()
        for piece in range(pieces):
            last_copy(1, piece).start()


    @pl.when(helper)
    def _():
        merge_rows()
        hear(0)
        tell(1)
        down_copy(everything).wait_recv()

    @pl.when(host)
    def _():
        merge_rows()

    own_rows()

    for hop in range(1, turns):
        hear(hop)
        tell(hop + 1)
    lane = lax.broadcasted_iota(jnp.int32, (tall, count), 1)

    def choose(values):
        result = values[0]
        for k in range(1, groups):
            result = jnp.where(lane < k * wide, result, values[k])
        return result

    for part in range(groups):
        for piece in range(part * pieces // groups, (part + 1) * pieces // groups):
            last_copy(1, piece).wait_recv()
        for low, high in ((0, quarter), (quarter, n_blk)):
            total = partial[low * owned : high * owned, :] + other_rows(part, low * owned, high * owned)
            for target in range(low, high):
                top = (target - low) * owned
                packed = choose(
                    [
                        total[top + g * tall : top + (g + 1) * tall]
                        for g in ((k - part) % groups for k in range(groups))
                    ]
                )
                outgoing[part, target] = packed.astype(BF16)
                scatter(part, target, False)
        incoming[part, block] = outgoing[part, block]
    for part in range(groups):
        for target in range(quarter, n_blk):
            scatter(part, target, True)

    def sent(index, which):
        source = held.at[index, which] if index == 0 else held.at[index]
        remote(source, source, stage_send.at[index], stage_recv.at[index, 0], mate).wait_send()

    first_copy.wait_send()
    sent(0, core)

    @pl.when(helper)
    def _():
        held_copy.wait_send()
        for index, stage in enumerate(stages):
            lower_copy(index).wait_send()
            if len(stage) == 2:
                upper_copy(index).wait_send()
                part = mixing.at[index, :, pl.ds(0, rank), pl.ds(0, rank)]
                remote(part, part, weight_sem.at[index, 4], weight_sem.at[index, 5], mate).wait_send()

    @pl.when(host)
    def _():
        for index in range(1, len(stages)):
            sent(index, 0)
        for which in range(2):
            whole = last.at[mine]
            remote(whole, whole, last_send.at[which], last_recv.at[0], mate).wait_send()
        down_copy(everything).wait_send()

    sums = []
    for part in range(groups):
        if part == groups - 1:
            whole = outgoing.at[:, others]
            remote(whole, whole, scatter_send.at[0], scatter_recv.at[0], mate).wait_send()
        whole = incoming.at[part, others]
        remote(whole, whole, scatter_send.at[0], scatter_recv.at[part], mate).wait_recv()
        total = incoming[part, 0].astype(F32)
        for source in range(1, n_blk):
            total = total + incoming[part, source].astype(F32)
        sums.append(total * (1.0 / math.sqrt(n_blk)))
    for g in range(groups):
        value = choose([sums[(k - g) % groups] for k in range(groups)])
        if g:
            value = pltpu.roll(value, (count - g * wide) % count, 1)
        out_ref[0, g * tall : (g + 1) * tall, :] = value.astype(BF16)


def solution(mesh):
    n_blk, n_bfly = mesh.shape["blk"], mesh.shape["bfly"]

    def local(port_vectors, column_leaf, transfer, row_leaf):
        _, _, leaf, ports = port_vectors.shape
        rank = column_leaf.shape[2]
        levels = transfer.shape[1]
        rows = row_leaf.shape[2]
        owned = rows // n_blk
        depth = len(plan(levels, n_bfly.bit_length() - 1)[1])
        assert n_blk % 4 == 0 and n_blk & (n_blk - 1) == 0
        dma = pltpu.SemaphoreType.DMA
        return pl.pallas_call(
            functools.partial(kernel, n_blk, n_bfly, PIECES, GROUPS),
            out_shape=pltpu.VMEM((1, owned, ports), BF16),
            in_specs=[pl.BlockSpec(memory_space=pl.ANY)] * 4,
            out_specs=pl.BlockSpec(memory_space=pltpu.VMEM),
            scratch_shapes=[
                pltpu.VMEM((leaf, ports), BF16),
                pltpu.VMEM((rank, leaf), BF16),
                pltpu.VMEM((levels, rank, 2 * rank), BF16),
                pltpu.VMEM((depth, rank, 2 * rank), BF16),
                pltpu.VMEM((depth, rank, rank), BF16),
                pltpu.VMEM((rows, rank), BF16),
                pltpu.VMEM((2, ports, rank), BF16),
                pltpu.VMEM((depth, 2, ports, rank), BF16),
                pltpu.VMEM((depth, 2, ports, rank), BF16),
                pltpu.VMEM((ports, 2 * rank), F32),
                pltpu.VMEM((2, 2 * rank, rank), BF16),
                pltpu.VMEM((depth, 2, 2 * rank, 2 * rank), BF16),
                pltpu.VMEM((ports, rank), BF16),
                pltpu.VMEM((2, ports, rank), BF16),
                pltpu.VMEM((GROUPS, n_blk, owned // GROUPS, ports), BF16),
                pltpu.VMEM((GROUPS, n_blk, owned // GROUPS, ports), BF16),
                pltpu.VMEM((rows, 2 * rank), BF16),
                pltpu.VMEM((rows, ports), F32),
                dma((levels + 3,)),
                dma((2,)),
                dma((depth, 7)),
                dma((2,)),
                dma((depth,)),
                dma((depth, PIECES)),
                dma((2,)),
                dma((PIECES,)),
                dma((2,)),
                dma((1,)),
                dma((GROUPS,)),
                pltpu.SemaphoreType.REGULAR((n_blk.bit_length(),)),
            ],
            compiler_params=pltpu.CompilerParams(collective_id=0, has_side_effects=True),
        )(port_vectors, column_leaf, transfer, row_leaf)

    placed = (
        P("blk", "bfly", None, None),
        P("blk", "bfly", None, None),
        P("blk", None, "bfly", None, None),
        P("blk", "bfly", None, None),
    )
    return jax.shard_map(
        local, mesh=mesh, in_specs=placed, out_specs=P("bfly", "blk", None), check_vma=False
    )
```

```python
import functools
import math

import jax
import jax.numpy as jnp
from jax import lax
from jax.experimental import pallas as pl
from jax.experimental.pallas import tpu as pltpu
from jax.sharding import PartitionSpec as P

PIECES = 4
GROUPS = 2
MESH = pl.DeviceIdType.MESH
F32 = jnp.float32
BF16 = jnp.bfloat16


def plan(levels, bit_count):
    bits = [level % bit_count for level in range(levels)]
    stages, level = [], 1
    while level < levels - 1:
        assert bits[level] > 0
        pair = level + 1 < levels - 1 and bits[level + 1] == 0
        stages.append((level, level + 1) if pair else (level,))
        level += len(stages[-1])
    assert stages and bits[levels - 1] > 0
    return bits, stages


def contract(left, right):
    return lax.dot_general(left, right, (((1,), (1,)), ((), ())), preferred_element_type=F32)


def kernel(
    n_blk, n_bfly, pieces, groups,
    ports_hbm, column_hbm, transfer_hbm, row_hbm, out_ref,
    ports, column, transfer, foreign, upper, row, first, held, arrived, begun, turned, mixing, lent,
    last, outgoing, incoming, merged, partial,
    load_sem, first_sem, weight_sem, held_sem, stage_send, stage_recv, last_send, last_recv, down_sem,
    scatter_send, scatter_recv, meet_sem,
):
    levels, rank, _ = transfer.shape
    count = ports.shape[1]
    leaf = row.shape[0]
    owned = leaf // n_blk
    bits, stages = plan(levels, n_bfly.bit_length() - 1)
    entry, final = stages[0][0], levels - 1
    block = lax.axis_index("blk")
    position = lax.axis_index("bfly")
    core = lax.rem(position, 2)
    host, helper = core == 1, core == 0
    width = count // pieces
    spans = [pl.ds(piece * width, width) for piece in range(pieces)]
    tall, wide, quarter = owned // groups, count // groups, n_blk // 4

    def load(source, target, sem):
        copy = pltpu.make_async_copy(source, target, sem)
        copy.start()
        return copy

    loads = [
        load(ports_hbm.at[0, 0], ports, load_sem.at[levels]),
        load(column_hbm.at[0, 0], column, load_sem.at[levels + 1]),
    ]
    transfer_loads = {
        level: load(transfer_hbm.at[0, level, 0], transfer.at[level], load_sem.at[level])
        for level in range(levels)
    }
    row_load = load(row_hbm.at[0, 0], row, load_sem.at[levels + 2])

    def side(which):
        return pl.ds(pl.multiple_of(which * rank, rank), rank)

    def bit_of(level):
        return lax.rem(position // 2 ** bits[level], 2)

    def across(level, to_core):
        place = position + (1 - 2 * bit_of(level)) * 2 ** bits[level]
        return {"bfly": place - core + to_core}

    def near_peers(distance):
        pair = block // 2
        return [
            (pair >= 0, {"blk": block + 1 - 2 * lax.rem(block, 2)}),
            (pair >= distance, {"blk": block - 2 * distance}),
            (pair + distance < n_blk // 2, {"blk": block + 2 * distance}),
        ]

    def number(peers):
        return sum(there.astype(jnp.int32) for there, _ in peers)

    mate = {"bfly": position + 1 - 2 * core}
    barrier = pltpu.get_barrier_semaphore()

    def greet(target):
        pl.semaphore_signal(barrier, inc=1, device_id=target, device_id_type=MESH)

    host_bits = {}
    for level in [stage[0] for stage in stages] + [final]:
        host_bits.setdefault(bits[level], level)
    mixed_bits = {bits[final]: final, bits[entry]: entry}
    greet(mate)
    for level in mixed_bits.values():
        greet(across(level, 1 - core))

    @pl.when(host)
    def _():
        for level in host_bits.values():
            greet(across(level, 1))

    near = near_peers(1)
    for there, peer in near:
        pl.when(there)(functools.partial(greet, peer))

    turns = (n_blk // 2).bit_length() - 1

    def tell(turn):
        if turn < turns:
            for there, peer in near_peers(2**turn):

                @pl.when(there)
                def _(peer=peer):
                    pl.semaphore_signal(meet_sem.at[turn], inc=1, device_id=peer, device_id_type=MESH)

    def hear(turn):
        if turn < turns:
            pl.semaphore_wait(meet_sem.at[turn], number(near_peers(2**turn)))

    def remote(source, target, send_sem, recv_sem, device):
        return pltpu.make_async_remote_copy(
            src_ref=source, dst_ref=target, send_sem=send_sem, recv_sem=recv_sem,
            device_id=device, device_id_type=MESH,
        )

    first_copy = remote(first.at[core], first.at[core], first_sem.at[0], first_sem.at[1], mate)
    held_copy = remote(held.at[0, 0], held.at[0, 0], held_sem.at[0], held_sem.at[1], mate)

    def lower_copy(index):
        return remote(
            transfer.at[stages[index][0]], foreign.at[index], weight_sem.at[index, 0], weight_sem.at[index, 1], mate
        )

    def upper_copy(index):
        return remote(
            transfer.at[stages[index][1], :, pl.ds(rank, rank)], upper.at[index], weight_sem.at[index, 2],
            weight_sem.at[index, 3], mate,
        )

    def mixing_copy(index, half):
        part = mixing.at[index, half, pl.ds(0, rank), pl.ds(0, rank)]
        return remote(part, part, weight_sem.at[index, 4], weight_sem.at[index, 5 + half], mate)

    def stage_start(index, which, piece):
        remote(
            held.at[index, which, spans[piece]], arrived.at[index, which, spans[piece]],
            stage_send.at[index], stage_recv.at[index, piece], across(stages[index][0], 1),
        ).start()

    def stage_arrival(index, piece):
        both = arrived.at[index, :, spans[piece]]
        return remote(both, both, stage_send.at[index], stage_recv.at[index, piece], mate)

    mine = bit_of(final)

    def last_copy(which, piece):
        source = lent.at[spans[piece]] if which == 0 else last.at[mine, spans[piece]]
        return remote(
            source, last.at[mine, spans[piece]], last_send.at[which], last_recv.at[piece * groups // pieces],
            across(final, which),
        )

    def down_copy(span):
        return remote(lent.at[span], last.at[mine, span], down_sem.at[0], down_sem.at[1], mate)

    everything, others = pl.ds(0, count), pl.ds(0, n_blk - 1)

    def scatter(part, target, late):
        ready = block != target
        if target >= quarter:
            far = block >= quarter
            ready = jnp.logical_and(ready, far if late else jnp.logical_not(far))
        elif late:
            return

        @pl.when(ready)
        def _():
            remote(
                outgoing.at[part, target], incoming.at[part, block], scatter_send.at[0], scatter_recv.at[part],
                {"blk": target},
            ).start()

    def own_rows():
        value = contract(merged[:, side(mine)], last[mine])
        for start in range(0, leaf, tall):
            shift = start // tall % groups * wide
            rows = value[start : start + tall]
            partial[start : start + tall, :] = pltpu.roll(rows, shift, 1) if shift else rows

    def other_rows(part, first_row, end_row):
        value = last[1 - mine, part * wide : (part + 1) * wide, :]
        return contract(merged[first_row:end_row, side(1 - mine)], jnp.concatenate([value] * groups, axis=0))

    def turn(index, slot, matrix):
        bit = bit_of(stages[index][0])
        for half, which in ((0, bit), (1, 1 - bit)):
            turned[slot, half * rank : (half + 1) * rank] = matrix[:, side(which)].T

    def join(index, slot, inner, outer, factor):
        both = contract(turned[slot], factor).astype(BF16)
        for half in range(2):
            mixing[index, half, side(inner), side(outer)] = both[half * rank : (half + 1) * rank]

    def join_own(index):
        low, high = stages[index]
        turn(index, 0, transfer.at[low])
        join(index, 0, core, core, transfer[high, :, side(core)])

    def merge_rows():
        transfer_loads[final].wait()
        row_load.wait()
        merged[...] = jnp.dot(row[...], transfer[final], preferred_element_type=F32).astype(BF16)

    loads[0].wait()
    loads[1].wait()
    state = lax.dot_general(ports[...], column[...], (((0,), (1,)), ((), ())), preferred_element_type=F32)
    first[core] = state.astype(BF16)
    pl.semaphore_wait(barrier, 1 + len(mixed_bits) + core * len(host_bits) + number(near))
    tell(0)
    first_copy.start()
    for level in range(final):
        transfer_loads[level].wait()

    @pl.when(helper)
    def _():
        lower_copy(0).start()

    own = contract(first[core], transfer[0, :, side(core)])
    if len(stages[0]) == 2:
        join_own(0)
    first_copy.wait_recv()
    state = own + contract(first[1 - core], transfer[0, :, side(1 - core)])
    held[0, core] = state.astype(BF16)
    for piece in range(pieces):
        stage_start(0, core, piece)
    @pl.when(helper)
    def _():
        held_copy.start()
        for index, stage in enumerate(stages):
            if index:
                lower_copy(index).start()
            if len(stage) == 2:
                upper_copy(index).start()
                if index:
                    join_own(index)
                for half in range(2):
                    mixing_copy(index, half).start()

    def mix(index, states, arriving):
        stage = stages[index]
        if len(stage) == 2:
            return jnp.dot(jnp.concatenate(states, axis=1), mixing[index, arriving], preferred_element_type=F32)
        bit = bit_of(stage[0])
        which = side(1 - bit if arriving else bit)
        factors = [foreign[index, :, which], transfer[stage[0], :, which]]
        return jnp.concatenate([contract(*pair) for pair in zip(states, factors)], axis=1)

    @pl.when(host)
    def _():
        for index, stage in enumerate(stages):
            if len(stage) == 2:
                if index:
                    join_own(index)
                lower_copy(index).wait_recv()
                turn(index, 1, foreign.at[index])
                join(index, 1, 0, 1, transfer[stage[1], :, :rank])
                upper_copy(index).wait_recv()
                join(index, 0, 1, 0, upper[index])
                mixing_copy(index, 0).wait_recv()
            else:
                lower_copy(index).wait_recv()
            if index == 0:
                held_copy.wait_recv()
            begun[...] = mix(index, [held[index, 0], held[index, 1]], 0)
            if index == 0:
                hear(0)
                tell(1)
            if len(stage) == 2:
                mixing_copy(index, 1).wait_recv()
            for piece in range(pieces):
                stage_arrival(index, piece).wait_recv()
                total = begun[spans[piece], :] + mix(
                    index, [arrived[index, 0, spans[piece], :], arrived[index, 1, spans[piece], :]], 1
                )
                total = total.astype(BF16)
                if index + 1 < len(stages):
                    for which in range(2):
                        held[index + 1, which, spans[piece], :] = total[:, which * rank : (which + 1) * rank]
                        stage_start(index + 1, which, piece)
                else:
                    lent[spans[piece], :] = total[:, :rank]
                    last_copy(0, piece).start()
                    last[mine, spans[piece], :] = total[:, rank:]
                    down_copy(spans[piece]).start()
        for piece in range(pieces):
            last_copy(1, piece).start()


    @pl.when(helper)
    def _():
        merge_rows()
        hear(0)
        tell(1)
        down_copy(everything).wait_recv()

    @pl.when(host)
    def _():
        merge_rows()

    own_rows()

    for hop in range(1, turns):
        hear(hop)
        tell(hop + 1)
    lane = lax.broadcasted_iota(jnp.int32, (tall, count), 1)

    def choose(values):
        result = values[0]
        for k in range(1, groups):
            result = jnp.where(lane < k * wide, result, values[k])
        return result

    for part in range(groups):
        whole = last.at[1 - mine, pl.ds(part * wide, wide)]
        remote(whole, whole, last_send.at[1], last_recv.at[part], mate).wait_recv()
        for low, high in ((0, quarter), (quarter, n_blk)):
            total = partial[low * owned : high * owned, :] + other_rows(part, low * owned, high * owned)
            for target in range(low, high):
                top = (target - low) * owned
                packed = choose(
                    [
                        total[top + g * tall : top + (g + 1) * tall]
                        for g in ((k - part) % groups for k in range(groups))
                    ]
                )
                outgoing[part, target] = packed.astype(BF16)
                scatter(part, target, False)
        incoming[part, block] = outgoing[part, block]
    for part in range(groups):
        for target in range(quarter, n_blk):
            scatter(part, target, True)

    def sent(index, which):
        source = held.at[index, which] if index == 0 else held.at[index]
        remote(source, source, stage_send.at[index], stage_recv.at[index, 0], mate).wait_send()

    first_copy.wait_send()
    sent(0, core)

    @pl.when(helper)
    def _():
        held_copy.wait_send()
        for index, stage in enumerate(stages):
            lower_copy(index).wait_send()
            if len(stage) == 2:
                upper_copy(index).wait_send()
                part = mixing.at[index, :, pl.ds(0, rank), pl.ds(0, rank)]
                remote(part, part, weight_sem.at[index, 4], weight_sem.at[index, 5], mate).wait_send()

    @pl.when(host)
    def _():
        for index in range(1, len(stages)):
            sent(index, 0)
        for which in range(2):
            whole = last.at[mine]
            remote(whole, whole, last_send.at[which], last_recv.at[0], mate).wait_send()
        down_copy(everything).wait_send()

    sums = []
    for part in range(groups):
        if part == groups - 1:
            whole = outgoing.at[:, others]
            remote(whole, whole, scatter_send.at[0], scatter_recv.at[0], mate).wait_send()
        whole = incoming.at[part, others]
        remote(whole, whole, scatter_send.at[0], scatter_recv.at[part], mate).wait_recv()
        total = incoming[part, 0].astype(F32)
        for source in range(1, n_blk):
            total = total + incoming[part, source].astype(F32)
        sums.append(total * (1.0 / math.sqrt(n_blk)))
    for g in range(groups):
        value = choose([sums[(k - g) % groups] for k in range(groups)])
        if g:
            value = pltpu.roll(value, (count - g * wide) % count, 1)
        out_ref[0, g * tall : (g + 1) * tall, :] = value.astype(BF16)


def solution(mesh):
    n_blk, n_bfly = mesh.shape["blk"], mesh.shape["bfly"]

    def local(port_vectors, column_leaf, transfer, row_leaf):
        _, _, leaf, ports = port_vectors.shape
        rank = column_leaf.shape[2]
        levels = transfer.shape[1]
        rows = row_leaf.shape[2]
        owned = rows // n_blk
        depth = len(plan(levels, n_bfly.bit_length() - 1)[1])
        assert n_blk % 4 == 0 and n_blk & (n_blk - 1) == 0
        dma = pltpu.SemaphoreType.DMA
        return pl.pallas_call(
            functools.partial(kernel, n_blk, n_bfly, PIECES, GROUPS),
            out_shape=pltpu.VMEM((1, owned, ports), BF16),
            in_specs=[pl.BlockSpec(memory_space=pl.ANY)] * 4,
            out_specs=pl.BlockSpec(memory_space=pltpu.VMEM),
            scratch_shapes=[
                pltpu.VMEM((leaf, ports), BF16),
                pltpu.VMEM((rank, leaf), BF16),
                pltpu.VMEM((levels, rank, 2 * rank), BF16),
                pltpu.VMEM((depth, rank, 2 * rank), BF16),
                pltpu.VMEM((depth, rank, rank), BF16),
                pltpu.VMEM((rows, rank), BF16),
                pltpu.VMEM((2, ports, rank), BF16),
                pltpu.VMEM((depth, 2, ports, rank), BF16),
                pltpu.VMEM((depth, 2, ports, rank), BF16),
                pltpu.VMEM((ports, 2 * rank), F32),
                pltpu.VMEM((2, 2 * rank, rank), BF16),
                pltpu.VMEM((depth, 2, 2 * rank, 2 * rank), BF16),
                pltpu.VMEM((ports, rank), BF16),
                pltpu.VMEM((2, ports, rank), BF16),
                pltpu.VMEM((GROUPS, n_blk, owned // GROUPS, ports), BF16),
                pltpu.VMEM((GROUPS, n_blk, owned // GROUPS, ports), BF16),
                pltpu.VMEM((rows, 2 * rank), BF16),
                pltpu.VMEM((rows, ports), F32),
                dma((levels + 3,)),
                dma((2,)),
                dma((depth, 7)),
                dma((2,)),
                dma((depth,)),
                dma((depth, PIECES)),
                dma((2,)),
                dma((GROUPS,)),
                dma((2,)),
                dma((1,)),
                dma((GROUPS,)),
                pltpu.SemaphoreType.REGULAR((n_blk.bit_length() - 2,)),
            ],
            compiler_params=pltpu.CompilerParams(collective_id=0, has_side_effects=True),
        )(port_vectors, column_leaf, transfer, row_leaf)

    placed = (
        P("blk", "bfly", None, None),
        P("blk", "bfly", None, None),
        P("blk", None, "bfly", None, None),
        P("blk", "bfly", None, None),
    )
    return jax.shard_map(
        local, mesh=mesh, in_specs=placed, out_specs=P("bfly", "blk", None), check_vma=False
    )
```
